32 devices in a mesh: dp: 4 (over z), row: 2 (over y), fsdp: 4 (over x, core).
Axes of the slice: x: 2, y: 2, z: 4, core: 2. Of those that a mesh axis runs over, the one named last changes fastest.
Arguments:
- x_in: bfloat16 [65536, 768], P(('dp', 'row', 'fsdp'))
- dy_out: bfloat16 [65536, 768], P(('dp', 'row', 'fsdp'))
- w_gate: bfloat16 [768, 2048], P(None, ('row', 'fsdp'))
- w_up: bfloat16 [768, 2048], P(None, ('row', 'fsdp'))
- w_down: bfloat16 [2048, 768], P(('row', 'fsdp'))
- g_next: float32 [32, 3, 768, 2048], P(('dp', 'row', 'fsdp'))
Outputs:
- output 1: bfloat16 [65536, 768], P(('dp', 'row', 'fsdp'))
- output 2: float32 [3, 768, 2048], P(None, None, ('row', 'fsdp'))
- output 3: float32 [32, 3, 768, 2048], P(('dp', 'row', 'fsdp'))
All inputs are finite; a program needn't handle non-finite values.
Results may differ from the reference program's by a relative error of at most 0.0139156.
Values are sent between devices in bfloat16 or wider.
A program may use at most 1 GiB of HBM per device.

```python
import jax
import jax.numpy as jnp
from jax import lax
import math

MODEL_DIM = 768
HIDDEN_DIM = 2048
TOKENS_DEV = 2048
DEVICES = 32


def setup_inputs(seed: int = 0) -> dict:
    rand_keys = jax.random.split(jax.random.key(seed), 6)
    act_shape = (DEVICES * TOKENS_DEV, MODEL_DIM)
    in_scale = 1.0 / math.sqrt(MODEL_DIM)
    hid_scale = 1.0 / math.sqrt(HIDDEN_DIM)
    x_in = jax.random.normal(rand_keys[0], act_shape, jnp.float32).astype(jnp.bfloat16)
    dy_out = jax.random.normal(rand_keys[1], act_shape, jnp.float32).astype(jnp.bfloat16)
    w_gate = (jax.random.normal(rand_keys[2], (MODEL_DIM, HIDDEN_DIM), jnp.float32) * in_scale).astype(jnp.bfloat16)
    w_up = (jax.random.normal(rand_keys[3], (MODEL_DIM, HIDDEN_DIM), jnp.float32) * in_scale).astype(jnp.bfloat16)
    w_down = (jax.random.normal(rand_keys[4], (HIDDEN_DIM, MODEL_DIM), jnp.float32) * hid_scale).astype(jnp.bfloat16)
    g_next = jax.random.normal(rand_keys[5], (DEVICES, 3, MODEL_DIM, HIDDEN_DIM), jnp.float32)
    return {"x_in": x_in, "dy_out": dy_out, "w_gate": w_gate, "w_up": w_up, "w_down": w_down, "g_next": g_next}


def local_backward(x_blk, dy_blk, w_gate, w_up, w_down):
    a_pre = jnp.dot(x_blk, w_gate, preferred_element_type=jnp.float32)
    b_pre = jnp.dot(x_blk, w_up, preferred_element_type=jnp.float32)
    sig_a = jax.nn.sigmoid(a_pre)
    silu_a = a_pre * sig_a
    h_act = (silu_a * b_pre).astype(jnp.bfloat16)
    dh_full = jnp.dot(dy_blk, w_down.T, preferred_element_type=jnp.float32)
    da_bf = (dh_full * b_pre * sig_a * (1.0 + a_pre * (1.0 - sig_a))).astype(jnp.bfloat16)
    db_bf = (dh_full * silu_a).astype(jnp.bfloat16)
    dx_acc = jnp.dot(da_bf, w_gate.T, preferred_element_type=jnp.float32) + jnp.dot(db_bf, w_up.T, preferred_element_type=jnp.float32)
    grad_gate = jnp.dot(x_blk.T, da_bf, preferred_element_type=jnp.float32)
    grad_up = jnp.dot(x_blk.T, db_bf, preferred_element_type=jnp.float32)
    grad_down = jnp.dot(dy_blk.T, h_act, preferred_element_type=jnp.float32)
    return dx_acc.astype(jnp.bfloat16), jnp.stack([grad_gate, grad_up, grad_down])


def reference(x_in, dy_out, w_gate, w_up, w_down, g_next):
    x_blocks = x_in.reshape(DEVICES, TOKENS_DEV, MODEL_DIM)
    dy_blocks = dy_out.reshape(DEVICES, TOKENS_DEV, MODEL_DIM)

    def per_device(block_pair):
        return local_backward(block_pair[0], block_pair[1], w_gate, w_up, w_down)

    dx_blocks, dw_local = lax.map(per_device, (x_blocks, dy_blocks))
    dx_in = dx_blocks.reshape(DEVICES * TOKENS_DEV, MODEL_DIM)
    dw_next = jnp.sum(g_next.astype(jnp.bfloat16).astype(jnp.float32), axis=0)
    return (dx_in, dw_next, dw_local)
```

```python
import functools

import jax
import jax.numpy as jnp
from jax import lax
from jax.experimental import pallas as pl
from jax.experimental.pallas import tpu as pltpu
from jax.sharding import PartitionSpec as P

ALL_AXES = ("dp", "row", "fsdp")
GROUP_AXES = ("row", "fsdp")
LAST = (((1,), (1,)), ((), ()))
F32, BF16 = jnp.float32, jnp.bfloat16

BLOCKS = 8
TILES = 4
UNITS = BLOCKS * TILES
CHUNKS = 18
FIRST = 4
LAGS = (0, 1, 3, 5, 7, 9, 11, 13)
FWD_XY, FWD_D = 6, 12
PASS = (13, 19, 25)
SLOTS = 4


def whole_step(x_hbm, dy_hbm, wg_hbm, wu_hbm, wd_hbm, g_hbm, dx_out, dn_out, dw_out,
               xv, dyv, xt, dyt, w1, w3, w2, dxacc, dwacc,
               gbuf, send_c, own, recv_c, recv_1, recv_2, recv_z1, recv_z2, res,
               ld_sem, g_sem, ws_sem, wr_sem, s_sem, r_sem, dw_sem, out_sem):
    z, y, f = lax.axis_index("dp"), lax.axis_index("row"), lax.axis_index("fsdp")
    x, c = f // 2, f % 2
    z0, z1 = z % 2, z // 2
    act = (z0 + c + 1) % 2
    tile = xv.shape[0] // TILES
    wide = w1.shape[2]
    half_w2 = w2.shape[1] // 2
    rows = gbuf.shape[1]
    rh, rq = rows // 2, rows // 4

    def dev(dz=None, yy=None, xx=None, cc=None):
        zz = z if dz is None else dz
        return (zz, y if yy is None else yy, (x if xx is None else xx) * 2 + (c if cc is None else cc))

    partner = dev(cc=1 - c)
    x_nbr, y_nbr = dev(xx=1 - x), dev(yy=1 - y)
    z_near = dev(dz=z + 1 - 2 * z0)
    z_far = dev(dz=(z + 2) % 4)

    own_loads = [pltpu.make_async_copy(s, d.at[0], ld_sem.at[i]) for i, (s, d) in enumerate(((wg_hbm, w1), (wu_hbm, w3), (wd_hbm, w2)))]
    act_loads = [pltpu.make_async_copy(s, d, ld_sem.at[3 + i]) for i, (s, d) in enumerate(((x_hbm, xv), (dy_hbm, dyv)))]
    for cp in own_loads + act_loads:
        cp.start()

    def g_load(k):
        return pltpu.make_async_copy(g_hbm.at[k], gbuf.at[k % 3], g_sem.at[k % 3])

    g_load(0).start()
    g_load(1).start()

    barrier = pltpu.get_barrier_semaphore()
    for d in (partner, x_nbr, y_nbr, z_near, z_far):
        pl.semaphore_signal(barrier, inc=1, device_id=d, device_id_type=pl.DeviceIdType.MESH)
    pl.semaphore_wait(barrier, 5)

    def part(slot, p):
        if p == 0:
            return w1.at[slot]
        if p == 1:
            return w3.at[slot]
        return w2.at[slot, pl.ds((p - 2) * half_w2, half_w2)]

    def wcopy(src, dst, p, sem, device):
        return pltpu.make_async_remote_copy(
            src_ref=part(src, p), dst_ref=part(dst, p), send_sem=ws_sem.at[sem, p], recv_sem=wr_sem.at[dst, p],
            device_id=device, device_id_type=pl.DeviceIdType.MESH)

    def wwait(slot, p):
        wcopy(slot, slot, p, 0, partner).wait_recv()

    def own_copies():
        return [wcopy(0, 1, p, 0, partner) for p in range(4)]

    def own_far():
        return [wcopy(0, s, p, i, d) for p in range(4) for s, i, d in ((2, 1, x_nbr), (3, 2, y_nbr))]

    def fwd_xy(p):
        near = [wcopy(2, 2, p, 3, z_near), wcopy(3, 3, p, 4, z_near), wcopy(2, 5, p, 5, partner), wcopy(3, 6, p, 6, partner)]
        if p % 2 == 0:
            return [wcopy(2, 4, p, 7, y_nbr)] + near
        return [wcopy(3, 4, p, 7, x_nbr)] + near

    def fwd_d(p):
        return [wcopy(4, 4, p, 8, z_near), wcopy(4, 7, p, 9, partner)]

    for cp in own_loads:
        cp.wait()
    for cp in own_copies():
        cp.start()

    @pl.when(act == 1)
    def _():
        for cp in own_far():
            cp.start()

    for cp in act_loads:
        cp.wait()

    def neighbour(k, stage):
        typ = (k + stage) % 2
        return dev(yy=(y + typ) % 2, xx=(x + 1 - typ) % 2)

    def rcopy(stage, k, src, dst, device):
        return pltpu.make_async_remote_copy(
            src_ref=src, dst_ref=dst, send_sem=s_sem.at[stage, k % SLOTS], recv_sem=r_sem.at[stage, k],
            device_id=device, device_id_type=pl.DeviceIdType.MESH)

    def stage_copy(stage, k):
        if stage == 0:
            return rcopy(0, k, send_c.at[k % SLOTS], recv_c.at[k], partner)
        if stage == 1:
            return rcopy(1, k, own.at[k, pl.ds(2, 2)], recv_1.at[k], neighbour(k, 0))
        if stage == 2:
            return rcopy(2, k, own.at[k, 1], recv_2.at[k], neighbour(k, 1))
        if stage == 3:
            return rcopy(3, k, own.at[k, 0, pl.ds((1 - z0) * rh, rh)], recv_z1.at[k], z_near)
        if stage == 4:
            return rcopy(4, k, own.at[k, 0, pl.ds(z0 * rh + (1 - z1) * rq, rq)], recv_z2.at[k], z_far)
        if stage == 5:
            mine = pl.ds(z0 * rh + z1 * rq, rq)
            return rcopy(5, k, res.at[k, mine], res.at[k, mine], z_far)
        mine = pl.ds(z0 * rh, rh)
        return rcopy(6, k, res.at[k, mine], res.at[k, mine], z_near)

    def send(stage, k):
        stage_copy(stage, k).start()

    def free_slot(stage, k):
        @pl.when(k >= SLOTS)
        def _():
            stage_copy(stage, k - SLOTS).wait_send()

    def add(p, q):
        return (p.astype(F32) + q.astype(F32)).astype(BF16)

    def event(stage, k):
        if stage < 7:
            free_slot(stage, k)
        if stage > 0:
            stage_copy(stage - 1, k).wait_recv()
        if stage == 0:
            typ = k % 2
            g_load(k).wait()

            @pl.when(k + 2 < CHUNKS)
            def _():
                g_load(k + 2).start()

            for a in range(2):
                for b in range(2):
                    xx = (x + a + (b - a) * typ) % 2
                    yy = (y + b + (a - b) * typ) % 2
                    block = yy * 4 + xx * 2
                    send_c[k % SLOTS, 2 * a + b] = gbuf[k % 3, :, pl.ds(pl.multiple_of((block + 1 - c) * wide, wide), wide)].astype(BF16)
                    own[k, 2 * a + b] = gbuf[k % 3, :, pl.ds(pl.multiple_of((block + c) * wide, wide), wide)].astype(BF16)
        elif stage == 1:
            own[k] = add(own[k], recv_c[k])
        elif stage == 2:
            own[k, 0:2] = add(own[k, 0:2], recv_1[k])
        elif stage == 3:
            own[k, 0] = add(own[k, 0], recv_2[k])
        elif stage == 4:
            at = pl.ds(pl.multiple_of(z0 * rh, rh), rh)
            own[k, 0, at] = add(own[k, 0, at], recv_z1[k])
        elif stage == 5:
            at = pl.ds(pl.multiple_of(z0 * rh + z1 * rq, rq), rq)
            res[k, at] = add(own[k, 0, at], recv_z2[k])
        if stage < 7:
            send(stage, k)

    def reduce_events(u):
        for stage in range(7, -1, -1):
            k = u - FIRST - LAGS[stage]

            @pl.when((k >= 0) & (k < CHUNKS))
            def _(stage=stage, k=k):
                event(stage, k)

    def weight_events(u):
        @pl.when((u == FWD_XY) & (act == 1))
        def _():
            for p in range(4):
                wwait(2, p)
                wwait(3, p)
                for cp in fwd_xy(p):
                    cp.start()

        @pl.when((u == FWD_D) & (act == 1))
        def _():
            for p in range(4):
                wwait(4, p)
                for cp in fwd_d(p):
                    cp.start()

        for i, when in enumerate(PASS):
            @pl.when((u == when) & (act == 0))
            def _(i=i):
                for p in range(4):
                    wwait(2 + i, p)
                    wcopy(2 + i, 5 + i, p, 3 + i, partner).start()

    def slot_of(i):
        return jnp.where(i < 2, i, 2 + (i + 1 + 3 * (1 - act) + 3) % 6)

    def column_of(slot):
        b = jnp.where(slot < 5, slot, slot - 3)
        dc = jnp.where((slot == 1) | (slot >= 5), 1, 0)
        ddx = jnp.where((b == 2) | (b == 4), 1, 0)
        ddy = jnp.where((b == 3) | (b == 4), 1, 0)
        return ((y + ddy) % 2) * 4 + ((x + ddx) % 2) * 2 + (c + dc) % 2

    def dw_copy(i):
        at = pl.ds(pl.multiple_of(column_of(slot_of(i)) * wide, wide), wide)
        return pltpu.make_async_copy(dwacc.at[i % 2], dw_out.at[:, :, at], dw_sem.at[i % 2])

    def dx_copy(m):
        at = pl.ds(pl.multiple_of(m * tile, tile), tile)
        return pltpu.make_async_copy(xv.at[at], dx_out.at[at], out_sem.at[m])

    def compute(u):
        i, m = u // TILES, u % TILES
        slot = slot_of(i)
        d = i % 2
        at = pl.ds(pl.multiple_of(m * tile, tile), tile)

        @pl.when((m == 0) & ((slot == 1) | (slot >= 5)))
        def _():
            for p in range(4):
                wwait(slot, p)

        @pl.when((m == 0) & (i >= 2))
        def _():
            dw_copy(i - 2).wait()

        @pl.when(i == 0)
        def _():
            xt[m] = xv[at].T
            dyt[m] = dyv[at].T

        dot = functools.partial(lax.dot_general, preferred_element_type=F32)
        a = jnp.dot(xv[at], w1[slot], preferred_element_type=F32)
        b = jnp.dot(xv[at], w3[slot], preferred_element_type=F32)
        dh = dot(dyv[at], w2[slot], LAST)
        s = jax.nn.sigmoid(a)
        silu = a * s
        h = (silu * b).astype(BF16)
        da = (dh * b * s * (1.0 + a * (1.0 - s))).astype(BF16)
        db = (dh * silu).astype(BF16)
        dx = dot(da, w1[slot], LAST) + dot(db, w3[slot], LAST)
        dxacc[at] = jnp.where(i == 0, 0.0, dxacc[at]) + dx
        for n, (left, right) in enumerate(((xt, da), (xt, db), (dyt, h))):
            dwacc[d, n] = jnp.where(m == 0, 0.0, dwacc[d, n]) + jnp.dot(left[m], right, preferred_element_type=F32)

        @pl.when(m == TILES - 1)
        def _():
            dw_copy(i).start()

        @pl.when(i == BLOCKS - 1)
        def _():
            xv[at] = dxacc[at].astype(BF16)
            dx_copy(m).start()

    def body(u, carry):
        weight_events(u)
        reduce_events(u)
        compute(u)
        return carry

    def tail(u, carry):
        reduce_events(u)
        return carry

    lax.fori_loop(0, UNITS, body, 0)
    lax.fori_loop(UNITS, FIRST + CHUNKS + LAGS[-1], tail, 0)

    store = pltpu.make_async_copy(res, dn_out, ld_sem.at[0])
    store.start()

    for cp in own_copies():
        cp.wait_send()

    @pl.when(act == 1)
    def _():
        for cp in own_far():
            cp.wait_send()
        for p in range(4):
            for cp in fwd_xy(p) + fwd_d(p):
                cp.wait_send()

    @pl.when(act == 0)
    def _():
        for i in range(3):
            for p in range(4):
                wcopy(2 + i, 5 + i, p, 3 + i, partner).wait_send()

    for stage in range(7):
        for k in range(CHUNKS - SLOTS, CHUNKS):
            stage_copy(stage, k).wait_send()
    dw_copy(BLOCKS - 2).wait()
    dw_copy(BLOCKS - 1).wait()
    for m in range(TILES):
        dx_copy(m).wait()
    store.wait()


def solution(mesh):
    def per_device(x_blk, dy_blk, gate, up, down, g_part):
        tokens, dim = x_blk.shape
        wide = gate.shape[1]
        hidden = wide * BLOCKS
        rows = 3 * dim // CHUNKS
        tile = tokens // TILES
        g = g_part.reshape(CHUNKS, rows, hidden)
        vm = pltpu.VMEM
        dma = pltpu.SemaphoreType.DMA
        dx, dn, dw = pl.pallas_call(
            whole_step,
            out_shape=[
                jax.ShapeDtypeStruct((tokens, dim), BF16),
                jax.ShapeDtypeStruct((CHUNKS, rows, wide), BF16),
                jax.ShapeDtypeStruct((3, dim, hidden), F32),
            ],
            in_specs=[pl.BlockSpec(memory_space=pl.ANY)] * 6,
            out_specs=[pl.BlockSpec(memory_space=pl.ANY)] * 3,
            scratch_shapes=[
                vm((tokens, dim), BF16), vm((tokens, dim), BF16),
                vm((TILES, dim, tile), BF16), vm((TILES, dim, tile), BF16),
                vm((BLOCKS, dim, wide), BF16), vm((BLOCKS, dim, wide), BF16), vm((BLOCKS, wide, dim), BF16),
                vm((tokens, dim), F32), vm((2, 3, dim, wide), F32),
                vm((3, rows, hidden), F32),
                vm((SLOTS, 4, rows, wide), BF16), vm((CHUNKS, 4, rows, wide), BF16), vm((CHUNKS, 4, rows, wide), BF16),
                vm((CHUNKS, 2, rows, wide), BF16), vm((CHUNKS, rows, wide), BF16),
                vm((CHUNKS, rows // 2, wide), BF16), vm((CHUNKS, rows // 4, wide), BF16), vm((CHUNKS, rows, wide), BF16),
                dma((5,)), dma((3,)), dma((10, 4)), dma((BLOCKS, 4)), dma((7, SLOTS)), dma((7, CHUNKS)), dma((2,)), dma((TILES,)),
            ],
            compiler_params=pltpu.CompilerParams(collective_id=0, has_side_effects=True, vmem_limit_bytes=67043328),
            cost_estimate=pl.CostEstimate(flops=16 * tokens * dim * hidden, bytes_accessed=60 << 20, transcendentals=tokens * hidden),
        )(x_blk, dy_blk, gate, up, down, g)
        return dx, dn.reshape(3, dim, wide).astype(F32), dw[None]

    return jax.shard_map(
        per_device,
        mesh=mesh,
        in_specs=(P(ALL_AXES, None), P(ALL_AXES, None), P(None, GROUP_AXES), P(None, GROUP_AXES), P(GROUP_AXES, None), P(ALL_AXES, None, None, None)),
        out_specs=(P(ALL_AXES, None), P(None, None, GROUP_AXES), P(ALL_AXES, None, None, None)),
        check_vma=False,
    )
```

```python
import functools

import jax
import jax.numpy as jnp
from jax import lax
from jax.experimental import pallas as pl
from jax.experimental.pallas import tpu as pltpu
from jax.sharding import PartitionSpec as P

ALL_AXES = ("dp", "row", "fsdp")
GROUP_AXES = ("row", "fsdp")
LAST = (((1,), (1,)), ((), ()))
F32, BF16 = jnp.float32, jnp.bfloat16

BLOCKS = 8
TILES = 4
UNITS = BLOCKS * TILES
CHUNKS = 18
FIRST = 4
LAGS = (0, 1, 3, 5, 8, 10, 12)
TAKE_XY, TAKE_D = (2, 4, 4, 6), (9, 9, 11, 15)
Z_X, Z_Y, Z_D = (2, 4, 4, 6), (5, 8, 11, 12), (10, 11, 13, 17)
PASS = ((9, 9, 13, 17), (14, 15, 18, 21), (17, 17, 21, 22))
GROUP = 4
SLOTS = 4


def whole_step(x_hbm, dy_hbm, wg_hbm, wu_hbm, wd_hbm, g_hbm, dx_out, dn_out, dw_out,
               xv, dyv, xt, dyt, w1, w3, w2, dxacc, dwacc,
               gbuf, send_c, own, recv_c, recv_1, recv_2, recv_z1, recv_z2, res,
               ld_sem, g_sem, ws_sem, wr_sem, s_sem, r_sem, dw_sem, out_sem):
    z, y, f = lax.axis_index("dp"), lax.axis_index("row"), lax.axis_index("fsdp")
    x, c = f // 2, f % 2
    z0, z1 = z % 2, z // 2
    act = (z0 + c + 1) % 2
    tile = xv.shape[0] // TILES
    wide = w1.shape[2]
    half_w2 = w2.shape[1] // 2
    rows = gbuf.shape[1]
    rh, rq = rows // 2, rows // 4

    def dev(dz=None, yy=None, xx=None, cc=None):
        zz = z if dz is None else dz
        return (zz, y if yy is None else yy, (x if xx is None else xx) * 2 + (c if cc is None else cc))

    partner = dev(cc=1 - c)
    x_nbr, y_nbr = dev(xx=1 - x), dev(yy=1 - y)
    z_near = dev(dz=z + 1 - 2 * z0)
    z_far = dev(dz=(z + 2) % 4)

    own_loads = [pltpu.make_async_copy(s, d.at[0], ld_sem.at[i]) for i, (s, d) in enumerate(((wg_hbm, w1), (wu_hbm, w3), (wd_hbm, w2)))]
    act_loads = [pltpu.make_async_copy(s, d, ld_sem.at[3 + i]) for i, (s, d) in enumerate(((x_hbm, xv), (dy_hbm, dyv)))]
    for cp in own_loads + act_loads:
        cp.start()

    def g_load(k):
        return pltpu.make_async_copy(g_hbm.at[k], gbuf.at[k % 3], g_sem.at[k % 3])

    g_load(0).start()
    g_load(1).start()

    barrier = pltpu.get_barrier_semaphore()
    for d in (partner, x_nbr, y_nbr, z_near, z_far):
        pl.semaphore_signal(barrier, inc=1, device_id=d, device_id_type=pl.DeviceIdType.MESH)
    pl.semaphore_wait(barrier, 5)

    def part(slot, p):
        if p == 0:
            return w1.at[slot]
        if p == 1:
            return w3.at[slot]
        return w2.at[slot, pl.ds((p - 2) * half_w2, half_w2)]

    def wcopy(src, dst, p, sem, device):
        return pltpu.make_async_remote_copy(
            src_ref=part(src, p), dst_ref=part(dst, p), send_sem=ws_sem.at[sem, p], recv_sem=wr_sem.at[dst, p],
            device_id=device, device_id_type=pl.DeviceIdType.MESH)

    def wwait(slot, p):
        wcopy(slot, slot, p, 0, partner).wait_recv()

    def own_copies():
        return [wcopy(0, 1, p, 0, partner) for p in range(4)]

    def own_far():
        return [wcopy(0, s, p, i, d) for p in range(4) for s, i, d in ((2, 1, x_nbr), (3, 2, y_nbr))]

    def z_x(p):
        return wcopy(2, 2, p, 3, z_near)

    def z_y(p):
        return wcopy(3, 3, p, 4, z_near)

    def z_d(p):
        return wcopy(4, 4, p, 8, z_near)

    def take_xy(p):
        diagonal = wcopy(2, 4, p, 7, y_nbr) if p % 2 == 0 else wcopy(3, 4, p, 7, x_nbr)
        return [diagonal, wcopy(2, 5, p, 5, partner), wcopy(3, 6, p, 6, partner)]

    def take_d(p):
        return wcopy(4, 7, p, 9, partner)

    def pass_on(i, p):
        return wcopy(2 + i, 5 + i, p, 3 + i, partner)

    fetch, relay = {}, {}
    for p in range(4):
        fetch.setdefault(TAKE_XY[p], []).append(((2, 3), functools.partial(take_xy, p), p))
        fetch.setdefault(TAKE_D[p], []).append(((4,), lambda p=p: [take_d(p)], p))
        for units, make in ((Z_X, z_x), (Z_Y, z_y), (Z_D, z_d)):
            fetch.setdefault(units[p], []).append(((), lambda p=p, make=make: [make(p)], p))
        for i in range(3):
            relay.setdefault(PASS[i][p], []).append(((2 + i,), lambda p=p, i=i: [pass_on(i, p)], p))

    for cp in own_loads:
        cp.wait()
    for cp in own_copies():
        cp.start()

    @pl.when(act == 1)
    def _():
        for cp in own_far():
            cp.start()

    for cp in act_loads:
        cp.wait()

    def neighbour(k, stage):
        typ = (k + stage) % 2
        return dev(yy=(y + typ) % 2, xx=(x + 1 - typ) % 2)

    def rcopy(stage, k, src, dst, device):
        return pltpu.make_async_remote_copy(
            src_ref=src, dst_ref=dst, send_sem=s_sem.at[stage, k % SLOTS], recv_sem=r_sem.at[stage, k],
            device_id=device, device_id_type=pl.DeviceIdType.MESH)

    def stage_copy(stage, k):
        if stage == 0:
            return rcopy(0, k, send_c.at[k % SLOTS], recv_c.at[k], partner)
        if stage == 1:
            return rcopy(1, k, own.at[k, pl.ds(2, 2)], recv_1.at[k], neighbour(k, 0))
        if stage == 2:
            return rcopy(2, k, own.at[k, 1], recv_2.at[k], neighbour(k, 1))
        if stage == 3:
            return rcopy(3, k, own.at[k, 0, pl.ds((1 - z0) * rh, rh)], recv_z1.at[k], z_near)
        if stage == 4:
            return rcopy(4, k, own.at[k, 0, pl.ds(z0 * rh + (1 - z1) * rq, rq)], recv_z2.at[k], z_far)
        if stage == 5:
            mine = pl.ds(z0 * rh + z1 * rq, rq)
            return rcopy(5, k, res.at[k, mine], res.at[k, mine], z_far)
        mine = pl.ds(z0 * rh, rh)
        return rcopy(6, k, res.at[k, mine], res.at[k, mine], z_near)

    def send(stage, k):
        stage_copy(stage, k).start()

    def free_slot(stage, k):
        @pl.when(k >= SLOTS)
        def _():
            stage_copy(stage, k - SLOTS).wait_send()

    def add(p, q):
        return (p.astype(F32) + q.astype(F32)).astype(BF16)

    def event(stage, k):
        free_slot(stage, k)
        if stage > 0:
            stage_copy(stage - 1, k).wait_recv()
        if stage == 0:
            typ = k % 2
            g_load(k).wait()

            @pl.when(k + 2 < CHUNKS)
            def _():
                g_load(k + 2).start()

            for a in range(2):
                for b in range(2):
                    xx = (x + a + (b - a) * typ) % 2
                    yy = (y + b + (a - b) * typ) % 2
                    block = yy * 4 + xx * 2
                    send_c[k % SLOTS, 2 * a + b] = gbuf[k % 3, :, pl.ds(pl.multiple_of((block + 1 - c) * wide, wide), wide)].astype(BF16)
                    own[k, 2 * a + b] = gbuf[k % 3, :, pl.ds(pl.multiple_of((block + c) * wide, wide), wide)].astype(BF16)
        elif stage == 1:
            own[k] = add(own[k], recv_c[k])
        elif stage == 2:
            own[k, 0:2] = add(own[k, 0:2], recv_1[k])
        elif stage == 3:
            own[k, 0] = add(own[k, 0], recv_2[k])
        elif stage == 4:
            at = pl.ds(pl.multiple_of(z0 * rh, rh), rh)
            own[k, 0, at] = add(own[k, 0, at], recv_z1[k])
        elif stage == 5:
            at = pl.ds(pl.multiple_of(z0 * rh + z1 * rq, rq), rq)
            res[k, at] = add(own[k, 0, at], recv_z2[k])
        send(stage, k)

    def reduce_events(u):
        for stage in range(6, -1, -1):
            k = u - FIRST - LAGS[stage]

            @pl.when((k >= 0) & (k < CHUNKS))
            def _(stage=stage, k=k):
                event(stage, k)

    def weight_events(u):
        for mine, table in ((1, fetch), (0, relay)):
            for group in sorted({t // GROUP for t in table}):
                @pl.when((u // GROUP == group) & (act == mine))
                def _(table=table, group=group):
                    for t in sorted(t for t in table if t // GROUP == group):
                        @pl.when(u == t)
                        def _(t=t):
                            for slots, make, p in table[t]:
                                for slot in slots:
                                    wwait(slot, p)
                                for cp in make():
                                    cp.start()

    def slot_of(i):
        return jnp.where(i < 2, i, 2 + (i + 1 + 3 * (1 - act) + 3) % 6)

    def column_of(slot):
        b = jnp.where(slot < 5, slot, slot - 3)
        dc = jnp.where((slot == 1) | (slot >= 5), 1, 0)
        ddx = jnp.where((b == 2) | (b == 4), 1, 0)
        ddy = jnp.where((b == 3) | (b == 4), 1, 0)
        return ((y + ddy) % 2) * 4 + ((x + ddx) % 2) * 2 + (c + dc) % 2

    def dw_copy(i):
        at = pl.ds(pl.multiple_of(column_of(slot_of(i)) * wide, wide), wide)
        return pltpu.make_async_copy(dwacc.at[i % 2], dw_out.at[:, :, at], dw_sem.at[i % 2])

    def dx_copy(m):
        at = pl.ds(pl.multiple_of(m * tile, tile), tile)
        return pltpu.make_async_copy(xv.at[at], dx_out.at[at], out_sem.at[m])

    def compute(u):
        i, m = u // TILES, u % TILES
        slot = slot_of(i)
        d = i % 2
        at = pl.ds(pl.multiple_of(m * tile, tile), tile)

        @pl.when((m == 0) & ((slot == 1) | (slot >= 5)))
        def _():
            for p in range(4):
                wwait(slot, p)

        @pl.when((m == 0) & (i >= 2))
        def _():
            dw_copy(i - 2).wait()

        @pl.when(i == 0)
        def _():
            xt[m] = xv[at].T
            dyt[m] = dyv[at].T

        dot = functools.partial(lax.dot_general, preferred_element_type=F32)
        a = jnp.dot(xv[at], w1[slot], preferred_element_type=F32)
        b = jnp.dot(xv[at], w3[slot], preferred_element_type=F32)
        dh = dot(dyv[at], w2[slot], LAST)
        s = jax.nn.sigmoid(a)
        silu = a * s
        h = (silu * b).astype(BF16)
        da = (dh * b * s * (1.0 + a * (1.0 - s))).astype(BF16)
        db = (dh * silu).astype(BF16)
        dx = dot(da, w1[slot], LAST) + dot(db, w3[slot], LAST)
        dxacc[at] = jnp.where(i == 0, 0.0, dxacc[at]) + dx
        for n, (left, right) in enumerate(((xt, da), (xt, db), (dyt, h))):
            dwacc[d, n] = jnp.where(m == 0, 0.0, dwacc[d, n]) + jnp.dot(left[m], right, preferred_element_type=F32)

        @pl.when(m == TILES - 1)
        def _():
            dw_copy(i).start()

        @pl.when(i == BLOCKS - 1)
        def _():
            xv[at] = dxacc[at].astype(BF16)
            dx_copy(m).start()

    def body(u, carry):
        weight_events(u)
        reduce_events(u)
        compute(u)
        return carry

    def tail(u, carry):
        reduce_events(u)
        return carry

    lax.fori_loop(0, UNITS, body, 0)
    lax.fori_loop(UNITS, FIRST + CHUNKS + LAGS[-1], tail, 0)

    for k in range(CHUNKS):
        stage_copy(6, k).wait_recv()
    store = pltpu.make_async_copy(res, dn_out, ld_sem.at[0])
    store.start()

    for cp in own_copies():
        cp.wait_send()

    @pl.when(act == 1)
    def _():
        for cp in own_far():
            cp.wait_send()
        for p in range(4):
            for cp in take_xy(p) + [take_d(p), z_x(p), z_y(p), z_d(p)]:
                cp.wait_send()

    @pl.when(act == 0)
    def _():
        for i in range(3):
            for p in range(4):
                pass_on(i, p).wait_send()

    for stage in range(7):
        for k in range(CHUNKS - SLOTS, CHUNKS):
            stage_copy(stage, k).wait_send()
    dw_copy(BLOCKS - 2).wait()
    dw_copy(BLOCKS - 1).wait()
    for m in range(TILES):
        dx_copy(m).wait()
    store.wait()


def solution(mesh):
    def per_device(x_blk, dy_blk, gate, up, down, g_part):
        tokens, dim = x_blk.shape
        wide = gate.shape[1]
        hidden = wide * BLOCKS
        rows = 3 * dim // CHUNKS
        tile = tokens // TILES
        g = g_part.reshape(CHUNKS, rows, hidden)
        vm = pltpu.VMEM
        dma = pltpu.SemaphoreType.DMA
        dx, dn, dw = pl.pallas_call(
            whole_step,
            out_shape=[
                jax.ShapeDtypeStruct((tokens, dim), BF16),
                jax.ShapeDtypeStruct((CHUNKS, rows, wide), BF16),
                jax.ShapeDtypeStruct((3, dim, hidden), F32),
            ],
            in_specs=[pl.BlockSpec(memory_space=pl.ANY)] * 6,
            out_specs=[pl.BlockSpec(memory_space=pl.ANY)] * 3,
            scratch_shapes=[
                vm((tokens, dim), BF16), vm((tokens, dim), BF16),
                vm((TILES, dim, tile), BF16), vm((TILES, dim, tile), BF16),
                vm((BLOCKS, dim, wide), BF16), vm((BLOCKS, dim, wide), BF16), vm((BLOCKS, wide, dim), BF16),
                vm((tokens, dim), F32), vm((2, 3, dim, wide), F32),
                vm((3, rows, hidden), F32),
                vm((SLOTS, 4, rows, wide), BF16), vm((CHUNKS, 4, rows, wide), BF16), vm((CHUNKS, 4, rows, wide), BF16),
                vm((CHUNKS, 2, rows, wide), BF16), vm((CHUNKS, rows, wide), BF16),
                vm((CHUNKS, rows // 2, wide), BF16), vm((CHUNKS, rows // 4, wide), BF16), vm((CHUNKS, rows, wide), BF16),
                dma((5,)), dma((3,)), dma((10, 4)), dma((BLOCKS, 4)), dma((7, SLOTS)), dma((7, CHUNKS)), dma((2,)), dma((TILES,)),
            ],
            compiler_params=pltpu.CompilerParams(collective_id=0, has_side_effects=True, vmem_limit_bytes=67043328),
            cost_estimate=pl.CostEstimate(flops=16 * tokens * dim * hidden, bytes_accessed=60 << 20, transcendentals=tokens * hidden),
        )(x_blk, dy_blk, gate, up, down, g)
        return dx, dn.reshape(3, dim, wide).astype(F32), dw[None]

    return jax.shard_map(
        per_device,
        mesh=mesh,
        in_specs=(P(ALL_AXES, None), P(ALL_AXES, None), P(None, GROUP_AXES), P(None, GROUP_AXES), P(GROUP_AXES, None), P(ALL_AXES, None, None, None)),
        out_specs=(P(ALL_AXES, None), P(None, None, GROUP_AXES), P(ALL_AXES, None, None, None)),
        check_vma=False,
    )
```

```python
import functools

import jax
import jax.numpy as jnp
from jax import lax
from jax.experimental import pallas as pl
from jax.experimental.pallas import tpu as pltpu
from jax.sharding import PartitionSpec as P

ALL_AXES = ("dp", "row", "fsdp")
GROUP_AXES = ("row", "fsdp")
LAST = (((1,), (1,)), ((), ()))
FIRST_TO_LAST = (((1,), (0,)), ((), ()))
F32, BF16 = jnp.float32, jnp.bfloat16

BLOCKS = 8
TILES = 4
UNITS = BLOCKS * TILES
CHUNKS = 18
FIRST = 4
LAGS = (0, 1, 3, 5, 8, 10, 12)
TAKE_XY, TAKE_D = (2, 4, 4, 6), (9, 9, 11, 15)
Z_X, Z_Y, Z_D = (2, 4, 4, 6), (5, 8, 11, 12), (10, 11, 13, 17)
PASS = ((9, 9, 13, 17), (14, 15, 18, 21), (17, 17, 21, 22))
GROUP = 4
SLOTS = 4


def whole_step(x_hbm, dy_hbm, wg_hbm, wu_hbm, wd_hbm, g_hbm, dx_out, dn_out, dw_out,
               xv, dyv, xt, dyt, w13, w2, dab_even, dab_odd, h_even, h_odd, dxacc, dwacc,
               gbuf, send_c, own, recv_c, recv_1, recv_2, recv_z1, recv_z2, res,
               ld_sem, g_sem, ws_sem, wr_sem, s_sem, r_sem, dw_sem, out_sem):
    z, y, f = lax.axis_index("dp"), lax.axis_index("row"), lax.axis_index("fsdp")
    x, c = f // 2, f % 2
    z0, z1 = z % 2, z // 2
    act = (z0 + c + 1) % 2
    tile = xv.shape[0] // TILES
    wide = w13.shape[2] // 2
    half_w2 = w2.shape[1] // 2
    rows = gbuf.shape[1]
    rh, rq = rows // 2, rows // 4

    def dev(dz=None, yy=None, xx=None, cc=None):
        zz = z if dz is None else dz
        return (zz, y if yy is None else yy, (x if xx is None else xx) * 2 + (c if cc is None else cc))

    partner = dev(cc=1 - c)
    x_nbr, y_nbr = dev(xx=1 - x), dev(yy=1 - y)
    z_near = dev(dz=z + 1 - 2 * z0)
    z_far = dev(dz=(z + 2) % 4)

    own_loads = [pltpu.make_async_copy(s, d, ld_sem.at[i]) for i, (s, d) in enumerate(((wg_hbm, w13.at[0, :, pl.ds(0, wide)]), (wu_hbm, w13.at[0, :, pl.ds(wide, wide)]), (wd_hbm, w2.at[0])))]
    act_loads = [pltpu.make_async_copy(s, d, ld_sem.at[3 + i]) for i, (s, d) in enumerate(((x_hbm, xv), (dy_hbm, dyv)))]
    for cp in own_loads + act_loads:
        cp.start()

    def g_load(k):
        return pltpu.make_async_copy(g_hbm.at[k], gbuf.at[k % 3], g_sem.at[k % 3])

    g_load(0).start()
    g_load(1).start()

    barrier = pltpu.get_barrier_semaphore()
    for d in (partner, x_nbr, y_nbr, z_near, z_far):
        pl.semaphore_signal(barrier, inc=1, device_id=d, device_id_type=pl.DeviceIdType.MESH)
    pl.semaphore_wait(barrier, 5)

    def part(slot, p):
        if p < 2:
            return w13.at[slot, :, pl.ds(p * wide, wide)]
        return w2.at[slot, pl.ds((p - 2) * half_w2, half_w2)]

    def wcopy(src, dst, p, sem, device):
        return pltpu.make_async_remote_copy(
            src_ref=part(src, p), dst_ref=part(dst, p), send_sem=ws_sem.at[sem, p], recv_sem=wr_sem.at[dst, p],
            device_id=device, device_id_type=pl.DeviceIdType.MESH)

    def wwait(slot, p):
        wcopy(slot, slot, p, 0, partner).wait_recv()

    def own_copies():
        return [wcopy(0, 1, p, 0, partner) for p in range(4)]

    def own_far():
        return [wcopy(0, s, p, i, d) for p in range(4) for s, i, d in ((2, 1, x_nbr), (3, 2, y_nbr))]

    def z_x(p):
        return wcopy(2, 2, p, 3, z_near)

    def z_y(p):
        return wcopy(3, 3, p, 4, z_near)

    def z_d(p):
        return wcopy(4, 4, p, 8, z_near)

    def take_xy(p):
        diagonal = wcopy(2, 4, p, 7, y_nbr) if p % 2 == 0 else wcopy(3, 4, p, 7, x_nbr)
        return [diagonal, wcopy(2, 5, p, 5, partner), wcopy(3, 6, p, 6, partner)]

    def take_d(p):
        return wcopy(4, 7, p, 9, partner)

    def pass_on(i, p):
        return wcopy(2 + i, 5 + i, p, 3 + i, partner)

    fetch, relay = {}, {}
    for p in range(4):
        fetch.setdefault(TAKE_XY[p], []).append(((2, 3), functools.partial(take_xy, p), p))
        fetch.setdefault(TAKE_D[p], []).append(((4,), lambda p=p: [take_d(p)], p))
        for units, make in ((Z_X, z_x), (Z_Y, z_y), (Z_D, z_d)):
            fetch.setdefault(units[p], []).append(((), lambda p=p, make=make: [make(p)], p))
        for i in range(3):
            relay.setdefault(PASS[i][p], []).append(((2 + i,), lambda p=p, i=i: [pass_on(i, p)], p))

    for cp in own_loads:
        cp.wait()
    for cp in own_copies():
        cp.start()

    @pl.when(act == 1)
    def _():
        for cp in own_far():
            cp.start()

    for cp in act_loads:
        cp.wait()

    def neighbour(k, stage):
        typ = (k + stage) % 2
        return dev(yy=(y + typ) % 2, xx=(x + 1 - typ) % 2)

    def rcopy(stage, k, src, dst, device):
        return pltpu.make_async_remote_copy(
            src_ref=src, dst_ref=dst, send_sem=s_sem.at[stage, k % SLOTS], recv_sem=r_sem.at[stage, k],
            device_id=device, device_id_type=pl.DeviceIdType.MESH)

    def stage_copy(stage, k):
        if stage == 0:
            return rcopy(0, k, send_c.at[k % SLOTS], recv_c.at[k], partner)
        if stage == 1:
            return rcopy(1, k, own.at[k, pl.ds(2, 2)], recv_1.at[k], neighbour(k, 0))
        if stage == 2:
            return rcopy(2, k, own.at[k, 1], recv_2.at[k], neighbour(k, 1))
        if stage == 3:
            return rcopy(3, k, own.at[k, 0, pl.ds((1 - z0) * rh, rh)], recv_z1.at[k], z_near)
        if stage == 4:
            return rcopy(4, k, own.at[k, 0, pl.ds(z0 * rh + (1 - z1) * rq, rq)], recv_z2.at[k], z_far)
        if stage == 5:
            mine = pl.ds(z0 * rh + z1 * rq, rq)
            return rcopy(5, k, res.at[k, mine], res.at[k, mine], z_far)
        mine = pl.ds(z0 * rh, rh)
        return rcopy(6, k, res.at[k, mine], res.at[k, mine], z_near)

    def send(stage, k):
        stage_copy(stage, k).start()

    def free_slot(stage, k):
        @pl.when(k >= SLOTS)
        def _():
            stage_copy(stage, k - SLOTS).wait_send()

    def add(p, q):
        return (p.astype(F32) + q.astype(F32)).astype(BF16)

    def event(stage, k):
        free_slot(stage, k)
        if stage > 0:
            stage_copy(stage - 1, k).wait_recv()
        if stage == 0:
            typ = k % 2
            g_load(k).wait()

            @pl.when(k + 2 < CHUNKS)
            def _():
                g_load(k + 2).start()

            for a in range(2):
                for b in range(2):
                    xx = (x + a + (b - a) * typ) % 2
                    yy = (y + b + (a - b) * typ) % 2
                    block = yy * 4 + xx * 2
                    send_c[k % SLOTS, 2 * a + b] = gbuf[k % 3, :, pl.ds(pl.multiple_of((block + 1 - c) * wide, wide), wide)].astype(BF16)
                    own[k, 2 * a + b] = gbuf[k % 3, :, pl.ds(pl.multiple_of((block + c) * wide, wide), wide)].astype(BF16)
        elif stage == 1:
            own[k] = add(own[k], recv_c[k])
        elif stage == 2:
            own[k, 0:2] = add(own[k, 0:2], recv_1[k])
        elif stage == 3:
            own[k, 0] = add(own[k, 0], recv_2[k])
        elif stage == 4:
            at = pl.ds(pl.multiple_of(z0 * rh, rh), rh)
            own[k, 0, at] = add(own[k, 0, at], recv_z1[k])
        elif stage == 5:
            at = pl.ds(pl.multiple_of(z0 * rh + z1 * rq, rq), rq)
            res[k, at] = add(own[k, 0, at], recv_z2[k])
        send(stage, k)

    def reduce_events(u):
        for stage in range(6, -1, -1):
            k = u - FIRST - LAGS[stage]

            @pl.when((k >= 0) & (k < CHUNKS))
            def _(stage=stage, k=k):
                event(stage, k)

    def weight_events(u):
        for mine, table in ((1, fetch), (0, relay)):
            for group in sorted({t // GROUP for t in table}):
                @pl.when((u // GROUP == group) & (act == mine))
                def _(table=table, group=group):
                    for t in sorted(t for t in table if t // GROUP == group):
                        @pl.when(u == t)
                        def _(t=t):
                            for slots, make, p in table[t]:
                                for slot in slots:
                                    wwait(slot, p)
                                for cp in make():
                                    cp.start()

    def slot_of(i):
        return jnp.where(i < 2, i, 2 + (i + 1 + 3 * (1 - act) + 3) % 6)

    def column_of(slot):
        b = jnp.where(slot < 5, slot, slot - 3)
        dc = jnp.where((slot == 1) | (slot >= 5), 1, 0)
        ddx = jnp.where((b == 2) | (b == 4), 1, 0)
        ddy = jnp.where((b == 3) | (b == 4), 1, 0)
        return ((y + ddy) % 2) * 4 + ((x + ddx) % 2) * 2 + (c + dc) % 2

    def dw_copy(i):
        at = pl.ds(pl.multiple_of(column_of(slot_of(i)) * wide, wide), wide)
        return pltpu.make_async_copy(dwacc.at[i % 2], dw_out.at[:, :, at], dw_sem.at[i % 2])

    def dx_copy(m):
        at = pl.ds(pl.multiple_of(m * tile, tile), tile)
        return pltpu.make_async_copy(xv.at[at], dx_out.at[at], out_sem.at[m])

    dot = functools.partial(lax.dot_general, preferred_element_type=F32)

    def rows_of(m):
        return pl.ds(pl.multiple_of(m * tile, tile), tile)

    def before(u):
        weight_events(u)
        reduce_events(u)
        i, m = u // TILES, u % TILES
        slot = slot_of(i)

        @pl.when((m == 0) & ((slot == 1) | (slot >= 5)))
        def _():
            for p in range(4):
                wwait(slot, p)

        @pl.when(i == 0)
        def _():
            xt[m] = xv[rows_of(m)].T
            dyt[m] = dyv[rows_of(m)].T

        @pl.when((m == 1) & (i >= 2))
        def _():
            dw_copy(i - 2).wait()

    def products(u):
        slot, at = slot_of(u // TILES), rows_of(u % TILES)
        half = tile // 2
        first = pl.multiple_of((u % TILES) * tile, tile)
        dh = [dot(dyv[pl.ds(first + n * half, half)], w2[slot], LAST) for n in range(2)]
        return dot(xv[at], w13[slot], FIRST_TO_LAST), jnp.concatenate(dh, axis=0)

    def gate(ab, dh, dab, h):
        a, b = ab[:, :wide], ab[:, wide:]
        s = jax.nn.sigmoid(a)
        silu = a * s
        h[...] = (silu * b).astype(BF16)
        dab[:, :wide] = (dh * b * s * (1.0 + a * (1.0 - s))).astype(BF16)
        dab[:, wide:] = (dh * silu).astype(BF16)

    def gradients(u, dab, h):
        i, m = u // TILES, u % TILES
        d = i % 2
        half, dim = tile // 2, xt.shape[1] // 2
        first = pl.multiple_of(m * tile, tile)
        for n in range(2):
            at = pl.ds(n * dim, dim)
            dwacc[d, 2, at] = jnp.where(m == 0, 0.0, dwacc[d, 2, at]) + dot(dyt[m, at], h[...], FIRST_TO_LAST)
        for n in range(2):
            at = pl.ds(first + n * half, half)
            dxacc[at] = jnp.where(i == 0, 0.0, dxacc[at]) + dot(dab[n * half:(n + 1) * half], w13[slot_of(i)], LAST)
        for n in range(2):
            at = pl.ds(n * dim, dim)
            left = dot(xt[m, at], dab[...], FIRST_TO_LAST)
            dwacc[d, 0, at] = jnp.where(m == 0, 0.0, dwacc[d, 0, at]) + left[:, :wide]
            dwacc[d, 1, at] = jnp.where(m == 0, 0.0, dwacc[d, 1, at]) + left[:, wide:]

    def after(u):
        i, m = u // TILES, u % TILES

        @pl.when(m == TILES - 1)
        def _():
            dw_copy(i).start()

        @pl.when(i == BLOCKS - 1)
        def _():
            at = rows_of(m)
            xv[at] = dxacc[at].astype(BF16)
            dx_copy(m).start()

    even, odd = (dab_even, h_even), (dab_odd, h_odd)

    def step(u, now, last):
        before(u)
        ab, dh = products(u)
        gradients(u - 1, *last)
        gate(ab, dh, *now)
        after(u - 1)

    def body(v, carry):
        step(2 * v + 1, odd, even)
        step(2 * v + 2, even, odd)
        return carry

    def tail(u, carry):
        reduce_events(u)
        return carry

    before(0)
    gate(*products(0), *even)
    lax.fori_loop(0, UNITS // 2 - 1, body, 0)
    step(UNITS - 1, odd, even)
    reduce_events(UNITS)
    gradients(UNITS - 1, *odd)
    after(UNITS - 1)
    lax.fori_loop(UNITS + 1, FIRST + CHUNKS + LAGS[-1], tail, 0)

    for k in range(CHUNKS):
        stage_copy(6, k).wait_recv()
    store = pltpu.make_async_copy(res, dn_out, ld_sem.at[0])
    store.start()

    for cp in own_copies():
        cp.wait_send()

    @pl.when(act == 1)
    def _():
        for cp in own_far():
            cp.wait_send()
        for p in range(4):
            for cp in take_xy(p) + [take_d(p), z_x(p), z_y(p), z_d(p)]:
                cp.wait_send()

    @pl.when(act == 0)
    def _():
        for i in range(3):
            for p in range(4):
                pass_on(i, p).wait_send()

    for stage in range(7):
        for k in range(CHUNKS - SLOTS, CHUNKS):
            stage_copy(stage, k).wait_send()
    dw_copy(BLOCKS - 2).wait()
    dw_copy(BLOCKS - 1).wait()
    for m in range(TILES):
        dx_copy(m).wait()
    store.wait()


def solution(mesh):
    def per_device(x_blk, dy_blk, gate, up, down, g_part):
        tokens, dim = x_blk.shape
        wide = gate.shape[1]
        hidden = wide * BLOCKS
        rows = 3 * dim // CHUNKS
        tile = tokens // TILES
        g = g_part.reshape(CHUNKS, rows, hidden)
        vm = pltpu.VMEM
        dma = pltpu.SemaphoreType.DMA
        dx, dn, dw = pl.pallas_call(
            whole_step,
            out_shape=[
                jax.ShapeDtypeStruct((tokens, dim), BF16),
                jax.ShapeDtypeStruct((CHUNKS, rows, wide), BF16),
                jax.ShapeDtypeStruct((3, dim, hidden), F32),
            ],
            in_specs=[pl.BlockSpec(memory_space=pl.ANY)] * 6,
            out_specs=[pl.BlockSpec(memory_space=pl.ANY)] * 3,
            scratch_shapes=[
                vm((tokens, dim), BF16), vm((tokens, dim), BF16),
                vm((TILES, dim, tile), BF16), vm((TILES, dim, tile), BF16),
                vm((BLOCKS, dim, 2 * wide), BF16), vm((BLOCKS, wide, dim), BF16),
                vm((tile, 2 * wide), BF16), vm((tile, 2 * wide), BF16), vm((tile, wide), BF16), vm((tile, wide), BF16),
                vm((tokens, dim), F32), vm((2, 3, dim, wide), F32),
                vm((3, rows, hidden), F32),
                vm((SLOTS, 4, rows, wide), BF16), vm((CHUNKS, 4, rows, wide), BF16), vm((CHUNKS, 4, rows, wide), BF16),
                vm((CHUNKS, 2, rows, wide), BF16), vm((CHUNKS, rows, wide), BF16),
                vm((CHUNKS, rows // 2, wide), BF16), vm((CHUNKS, rows // 4, wide), BF16), vm((CHUNKS, rows, wide), BF16),
                dma((5,)), dma((3,)), dma((10, 4)), dma((BLOCKS, 4)), dma((7, SLOTS)), dma((7, CHUNKS)), dma((2,)), dma((TILES,)),
            ],
            compiler_params=pltpu.CompilerParams(collective_id=0, has_side_effects=True, vmem_limit_bytes=67043328),
            cost_estimate=pl.CostEstimate(flops=16 * tokens * dim * hidden, bytes_accessed=60 << 20, transcendentals=tokens * hidden),
        )(x_blk, dy_blk, gate, up, down, g)
        return dx, dn.reshape(3, dim, wide).astype(F32), dw[None]

    return jax.shard_map(
        per_device,
        mesh=mesh,
        in_specs=(P(ALL_AXES, None), P(ALL_AXES, None), P(None, GROUP_AXES), P(None, GROUP_AXES), P(GROUP_AXES, None), P(ALL_AXES, None, None, None)),
        out_specs=(P(ALL_AXES, None), P(None, None, GROUP_AXES), P(ALL_AXES, None, None, None)),
        check_vma=False,
    )
```

```python
import functools

import jax
import jax.numpy as jnp
from jax import lax
from jax.experimental import pallas as pl
from jax.experimental.pallas import tpu as pltpu
from jax.sharding import PartitionSpec as P

ALL_AXES = ("dp", "row", "fsdp")
GROUP_AXES = ("row", "fsdp")
LAST = (((1,), (1,)), ((), ()))
FIRST_TO_LAST = (((1,), (0,)), ((), ()))
F32, BF16 = jnp.float32, jnp.bfloat16

BLOCKS = 8
TILES = 4
UNITS = BLOCKS * TILES
CHUNKS = 18
FIRST = 5
LAGS = (0, 2, 4, 6, 10)
TAKE_XY, TAKE_D = (3, 4, 6, 6), (9, 10, 11, 14)
Z_X, Z_Y = (3, 4, 8, 10), (4, 7, 9, 13)
PASS_X, PASS_Y, PASS_D = (11, 13, 15, 16), (13, 14, 17, 17), (24, 25, 26, 27)
GROUP = 4
SLOTS = 4


def whole_step(x_hbm, dy_hbm, wg_hbm, wu_hbm, wd_hbm, g_hbm, dx_out, dn_out, dw_out,
               xv, dyv, xt, dyt, w13, w2, dab_even, dab_odd, h_even, h_odd, dxacc, dwacc,
               gbuf, send_c, own, recv_c, recv_1, recv_2, recv_z, res,
               ld_sem, g_sem, ws_sem, wr_sem, s_sem, r_sem, dw_sem, out_sem):
    z, y, f = lax.axis_index("dp"), lax.axis_index("row"), lax.axis_index("fsdp")
    x, c = f // 2, f % 2
    z0, z1 = z % 2, z // 2
    act = (z0 + c + 1) % 2
    tile = xv.shape[0] // TILES
    wide = w13.shape[2] // 2
    half_w2 = w2.shape[1] // 2
    rows = gbuf.shape[1]
    rq = rows // 4

    def dev(dz=None, yy=None, xx=None, cc=None):
        zz = z if dz is None else dz
        return (zz, y if yy is None else yy, (x if xx is None else xx) * 2 + (c if cc is None else cc))

    partner = dev(cc=1 - c)
    x_nbr, y_nbr = dev(xx=1 - x), dev(yy=1 - y)
    z_near = dev(dz=z + 1 - 2 * z0)
    others = [dev(dz=(z + j) % 4) for j in (1, 2, 3)]

    own_loads = [pltpu.make_async_copy(s, d, ld_sem.at[i]) for i, (s, d) in enumerate(((wg_hbm, w13.at[0, :, pl.ds(0, wide)]), (wu_hbm, w13.at[0, :, pl.ds(wide, wide)]), (wd_hbm, w2.at[0])))]
    act_loads = [pltpu.make_async_copy(s, d, ld_sem.at[3 + i]) for i, (s, d) in enumerate(((x_hbm, xv), (dy_hbm, dyv)))]
    for cp in own_loads + act_loads:
        cp.start()

    def g_load(k):
        return pltpu.make_async_copy(g_hbm.at[k], gbuf.at[k % 3], g_sem.at[k % 3])

    g_load(0).start()
    g_load(1).start()

    barrier = pltpu.get_barrier_semaphore()
    for d in (partner, x_nbr, y_nbr, *others):
        pl.semaphore_signal(barrier, inc=1, device_id=d, device_id_type=pl.DeviceIdType.MESH)
    pl.semaphore_wait(barrier, 6)

    def part(slot, p):
        if p < 2:
            return w13.at[slot, :, pl.ds(p * wide, wide)]
        return w2.at[slot, pl.ds((p - 2) * half_w2, half_w2)]

    def wcopy(src, dst, p, sem, device):
        return pltpu.make_async_remote_copy(
            src_ref=part(src, p), dst_ref=part(dst, p), send_sem=ws_sem.at[sem, p], recv_sem=wr_sem.at[dst, p],
            device_id=device, device_id_type=pl.DeviceIdType.MESH)

    def wwait(slot, p):
        wcopy(slot, slot, p, 0, partner).wait_recv()

    def own_copies():
        return [wcopy(0, 1, p, 0, partner) for p in range(4)]

    def own_far():
        return [wcopy(0, s, p, i, d) for p in range(4) for s, i, d in ((2, 1, x_nbr), (3, 2, y_nbr))]

    def z_x(p):
        return wcopy(2, 2, p, 3, z_near)

    def z_y(p):
        return wcopy(3, 3, p, 4, z_near)

    def take_x(p):
        return [wcopy(2, 5, p, 5, partner)] + ([wcopy(2, 4, p, 7, y_nbr)] if p % 2 == 0 else [])

    def take_y(p):
        return [wcopy(3, 6, p, 6, partner)] + ([wcopy(3, 4, p, 7, x_nbr)] if p % 2 == 1 else [])

    def take_d(p):
        return [wcopy(4, 7, p, 8, partner)]

    fetch, relay = {}, {}
    for p in range(4):
        fetch.setdefault(TAKE_XY[p], []).append((2, functools.partial(take_x, p), p))
        fetch.setdefault(TAKE_XY[p], []).append((3, functools.partial(take_y, p), p))
        for units, make in ((Z_X, z_x), (Z_Y, z_y)):
            fetch.setdefault(units[p], []).append((None, lambda p=p, make=make: [make(p)], p))
        relay.setdefault(PASS_X[p], []).append((2, functools.partial(take_x, p), p))
        relay.setdefault(PASS_Y[p], []).append((3, functools.partial(take_y, p), p))
        fetch.setdefault(TAKE_D[p], []).append((4, functools.partial(take_d, p), p))
        relay.setdefault(PASS_D[p], []).append((4, functools.partial(take_d, p), p))

    for cp in own_loads:
        cp.wait()
    for cp in own_copies():
        cp.start()

    @pl.when(act == 1)
    def _():
        for cp in own_far():
            cp.start()

    for cp in act_loads:
        cp.wait()

    def neighbour(k, stage):
        typ = (k + stage) % 2
        return dev(yy=(y + typ) % 2, xx=(x + 1 - typ) % 2)

    def rcopy(stage, k, src, dst, device):
        return pltpu.make_async_remote_copy(
            src_ref=src, dst_ref=dst, send_sem=s_sem.at[stage, k % SLOTS], recv_sem=r_sem.at[stage, k],
            device_id=device, device_id_type=pl.DeviceIdType.MESH)

    def quarter(zz):
        return pl.ds(pl.multiple_of(zz % 4 * rq, rq), rq)

    def stage_copy(stage, k):
        if stage == 0:
            return rcopy(0, k, send_c.at[k % SLOTS], recv_c.at[k], partner)
        if stage == 1:
            return rcopy(1, k, own.at[k, pl.ds(2, 2)], recv_1.at[k], neighbour(k, 0))
        if stage == 2:
            return rcopy(2, k, own.at[k, 1], recv_2.at[k], neighbour(k, 1))
        if stage < 6:
            j = stage - 3
            return rcopy(stage, k, own.at[k, 0, quarter(z + j + 1)], recv_z.at[k, j], others[j])
        return rcopy(stage, k, res.at[k, quarter(z)], res.at[k, quarter(z)], others[stage - 6])

    STARTS = ((0,), (1,), (2,), (3, 4, 5), (6, 7, 8))
    NEEDS = ((), (0,), (1,), (2,), (3, 4, 5))

    def free_slot(stage, k):
        @pl.when(k >= SLOTS)
        def _():
            stage_copy(stage, k - SLOTS).wait_send()

    def add(p, q):
        return (p.astype(F32) + q.astype(F32)).astype(BF16)

    def event(stage, k):
        for n in STARTS[stage]:
            free_slot(n, k)
        for n in NEEDS[stage]:
            stage_copy(n, k).wait_recv()
        if stage == 0:
            typ = k % 2
            g_load(k).wait()

            @pl.when(k + 2 < CHUNKS)
            def _():
                g_load(k + 2).start()

            for a in range(2):
                for b in range(2):
                    xx = (x + a + (b - a) * typ) % 2
                    yy = (y + b + (a - b) * typ) % 2
                    block = yy * 4 + xx * 2
                    send_c[k % SLOTS, 2 * a + b] = gbuf[k % 3, :, pl.ds(pl.multiple_of((block + 1 - c) * wide, wide), wide)].astype(BF16)
                    own[k, 2 * a + b] = gbuf[k % 3, :, pl.ds(pl.multiple_of((block + c) * wide, wide), wide)].astype(BF16)
        elif stage == 1:
            own[k] = add(own[k], recv_c[k])
        elif stage == 2:
            own[k, 0:2] = add(own[k, 0:2], recv_1[k])
        elif stage == 3:
            own[k, 0] = add(own[k, 0], recv_2[k])
        else:
            total = own[k, 0, quarter(z)].astype(F32)
            for j in range(3):
                total += recv_z[k, j].astype(F32)
            res[k, quarter(z)] = total.astype(BF16)
        for n in STARTS[stage]:
            stage_copy(n, k).start()

    def reduce_events(u):
        for stage in range(4, -1, -1):
            k = u - FIRST - LAGS[stage]

            @pl.when((k >= 0) & (k < CHUNKS))
            def _(stage=stage, k=k):
                event(stage, k)

    def weight_events(u):
        for mine, table in ((1, fetch), (0, relay)):
            for group in sorted({t // GROUP for t in table}):
                @pl.when((u // GROUP == group) & (act == mine))
                def _(table=table, group=group):
                    for t in sorted(t for t in table if t // GROUP == group):
                        @pl.when(u == t)
                        def _(t=t):
                            for slot, make, p in table[t]:
                                if slot is not None:
                                    wwait(slot, p)
                                for cp in make():
                                    cp.start()

    def slot_of(i):
        return jnp.where(i < 2, i, 2 + (i + 1 + 3 * (1 - act) + 3) % 6)

    def column_of(slot):
        b = jnp.where(slot < 5, slot, slot - 3)
        dc = jnp.where((slot == 1) | (slot >= 5), 1, 0)
        ddx = jnp.where((b == 2) | (b == 4), 1, 0)
        ddy = jnp.where((b == 3) | (b == 4), 1, 0)
        return ((y + ddy) % 2) * 4 + ((x + ddx) % 2) * 2 + (c + dc) % 2

    def dw_copy(i):
        at = pl.ds(pl.multiple_of(column_of(slot_of(i)) * wide, wide), wide)
        return pltpu.make_async_copy(dwacc.at[i % 2], dw_out.at[:, :, at], dw_sem.at[i % 2])

    def dx_copy(m):
        at = pl.ds(pl.multiple_of(m * tile, tile), tile)
        return pltpu.make_async_copy(xv.at[at], dx_out.at[at], out_sem.at[m])

    dot = functools.partial(lax.dot_general, preferred_element_type=F32)

    def rows_of(m):
        return pl.ds(pl.multiple_of(m * tile, tile), tile)

    def before(u):
        weight_events(u)
        reduce_events(u)
        i, m = u // TILES, u % TILES
        slot = slot_of(i)

        @pl.when((m == 0) & ((slot == 1) | (slot >= 5)))
        def _():
            for p in range(4):
                wwait(slot, p)

        @pl.when(i == 0)
        def _():
            xt[m] = xv[rows_of(m)].T
            dyt[m] = dyv[rows_of(m)].T

        @pl.when((m == 1) & (i >= 2))
        def _():
            dw_copy(i - 2).wait()

    def products(u):
        slot, at = slot_of(u // TILES), rows_of(u % TILES)
        half = tile // 2
        first = pl.multiple_of((u % TILES) * tile, tile)
        dh = [dot(dyv[pl.ds(first + n * half, half)], w2[slot], LAST) for n in range(2)]
        return dot(xv[at], w13[slot], FIRST_TO_LAST), jnp.concatenate(dh, axis=0)

    def gate(ab, dh, dab, h):
        a, b = ab[:, :wide], ab[:, wide:]
        s = jax.nn.sigmoid(a)
        silu = a * s
        h[...] = (silu * b).astype(BF16)
        dab[:, :wide] = (dh * b * s * (1.0 + a * (1.0 - s))).astype(BF16)
        dab[:, wide:] = (dh * silu).astype(BF16)

    def gradients(u, dab, h):
        i, m = u // TILES, u % TILES
        d = i % 2
        half, dim = tile // 2, xt.shape[1] // 2
        first = pl.multiple_of(m * tile, tile)
        for n in range(2):
            at = pl.ds(n * dim, dim)
            dwacc[d, 2, at] = jnp.where(m == 0, 0.0, dwacc[d, 2, at]) + dot(dyt[m, at], h[...], FIRST_TO_LAST)
        for n in range(2):
            at = pl.ds(first + n * half, half)
            dxacc[at] = jnp.where(i == 0, 0.0, dxacc[at]) + dot(dab[n * half:(n + 1) * half], w13[slot_of(i)], LAST)
        for n in range(2):
            at = pl.ds(n * dim, dim)
            left = dot(xt[m, at], dab[...], FIRST_TO_LAST)
            dwacc[d, 0, at] = jnp.where(m == 0, 0.0, dwacc[d, 0, at]) + left[:, :wide]
            dwacc[d, 1, at] = jnp.where(m == 0, 0.0, dwacc[d, 1, at]) + left[:, wide:]

    def after(u):
        i, m = u // TILES, u % TILES

        @pl.when(m == TILES - 1)
        def _():
            dw_copy(i).start()

        @pl.when(i == BLOCKS - 1)
        def _():
            at = rows_of(m)
            xv[at] = dxacc[at].astype(BF16)
            dx_copy(m).start()

    even, odd = (dab_even, h_even), (dab_odd, h_odd)

    def step(u, now, last):
        before(u)
        ab, dh = products(u)
        gradients(u - 1, *last)
        gate(ab, dh, *now)
        after(u - 1)

    def body(v, carry):
        step(2 * v + 1, odd, even)
        step(2 * v + 2, even, odd)
        return carry

    def tail(u, carry):
        reduce_events(u)
        return carry

    before(0)
    gate(*products(0), *even)
    lax.fori_loop(0, UNITS // 2 - 1, body, 0)
    step(UNITS - 1, odd, even)
    reduce_events(UNITS)
    gradients(UNITS - 1, *odd)
    after(UNITS - 1)
    lax.fori_loop(UNITS + 1, FIRST + CHUNKS + LAGS[-1], tail, 0)

    for k in range(CHUNKS):
        for n in (6, 7, 8):
            stage_copy(n, k).wait_recv()
    store = pltpu.make_async_copy(res, dn_out, ld_sem.at[0])
    store.start()

    for cp in own_copies():
        cp.wait_send()

    @pl.when(act == 1)
    def _():
        for cp in own_far():
            cp.wait_send()
        for p in range(4):
            z_x(p).wait_send()
            z_y(p).wait_send()

    for p in range(4):
        for cp in take_x(p) + take_y(p) + take_d(p):
            cp.wait_send()
    for stage in range(9):
        for k in range(CHUNKS - SLOTS, CHUNKS):
            stage_copy(stage, k).wait_send()
    dw_copy(BLOCKS - 2).wait()
    dw_copy(BLOCKS - 1).wait()
    for m in range(TILES):
        dx_copy(m).wait()
    store.wait()


def solution(mesh):
    def per_device(x_blk, dy_blk, gate, up, down, g_part):
        tokens, dim = x_blk.shape
        wide = gate.shape[1]
        hidden = wide * BLOCKS
        rows = 3 * dim // CHUNKS
        tile = tokens // TILES
        g = g_part.reshape(CHUNKS, rows, hidden)
        vm = pltpu.VMEM
        dma = pltpu.SemaphoreType.DMA
        dx, dn, dw = pl.pallas_call(
            whole_step,
            out_shape=[
                jax.ShapeDtypeStruct((tokens, dim), BF16),
                jax.ShapeDtypeStruct((CHUNKS, rows, wide), BF16),
                jax.ShapeDtypeStruct((3, dim, hidden), F32),
            ],
            in_specs=[pl.BlockSpec(memory_space=pl.ANY)] * 6,
            out_specs=[pl.BlockSpec(memory_space=pl.ANY)] * 3,
            scratch_shapes=[
                vm((tokens, dim), BF16), vm((tokens, dim), BF16),
                vm((TILES, dim, tile), BF16), vm((TILES, dim, tile), BF16),
                vm((BLOCKS, dim, 2 * wide), BF16), vm((BLOCKS, wide, dim), BF16),
                vm((tile, 2 * wide), BF16), vm((tile, 2 * wide), BF16), vm((tile, wide), BF16), vm((tile, wide), BF16),
                vm((tokens, dim), F32), vm((2, 3, dim, wide), F32),
                vm((3, rows, hidden), F32),
                vm((SLOTS, 4, rows, wide), BF16), vm((CHUNKS, 4, rows, wide), BF16), vm((CHUNKS, 4, rows, wide), BF16),
                vm((CHUNKS, 2, rows, wide), BF16), vm((CHUNKS, rows, wide), BF16),
                vm((CHUNKS, 3, rows // 4, wide), BF16), vm((CHUNKS, rows, wide), BF16),
                dma((5,)), dma((3,)), dma((10, 4)), dma((BLOCKS, 4)), dma((9, SLOTS)), dma((9, CHUNKS)), dma((2,)), dma((TILES,)),
            ],
            compiler_params=pltpu.CompilerParams(collective_id=0, has_side_effects=True, vmem_limit_bytes=67043328),
            cost_estimate=pl.CostEstimate(flops=16 * tokens * dim * hidden, bytes_accessed=60 << 20, transcendentals=tokens * hidden),
        )(x_blk, dy_blk, gate, up, down, g)
        return dx, dn.reshape(3, dim, wide).astype(F32), dw[None]

    return jax.shard_map(
        per_device,
        mesh=mesh,
        in_specs=(P(ALL_AXES, None), P(ALL_AXES, None), P(None, GROUP_AXES), P(None, GROUP_AXES), P(GROUP_AXES, None), P(ALL_AXES, None, None, None)),
        out_specs=(P(ALL_AXES, None), P(None, None, GROUP_AXES), P(ALL_AXES, None, None, None)),
        check_vma=False,
    )
```

```python
import functools

import jax
import jax.numpy as jnp
from jax import lax
from jax.experimental import pallas as pl
from jax.experimental.pallas import tpu as pltpu
from jax.sharding import PartitionSpec as P

ALL_AXES = ("dp", "row", "fsdp")
GROUP_AXES = ("row", "fsdp")
LAST = (((1,), (1,)), ((), ()))
FIRST_TO_LAST = (((1,), (0,)), ((), ()))
F32, BF16 = jnp.float32, jnp.bfloat16

BLOCKS = 8
TILES = 4
UNITS = BLOCKS * TILES
CHUNKS = 18
FIRST = 1
LAGS = (0, 1, 4, 7, 11, 13, 15)
TAKE_XY, TAKE_D = (2, 3, 4, 6), (10, 11, 14, 14)
Z_X, Z_Y = (2, 3, 4, 6), (4, 6, 10, 15)
PASS_X, PASS_Y, PASS_D = (10, 10, 13, 13), (14, 14, 16, 17), (22, 25, 27, 27)
GROUP = 4
SLOTS = 4


def whole_step(x_hbm, dy_hbm, wg_hbm, wu_hbm, wd_hbm, g_hbm, dx_out, dn_out, dw_out,
               xv, dyv, xt, dyt, w13, w2, dab_even, dab_odd, h_even, h_odd, dxacc, dwacc,
               gbuf, send_c, own, recv_c, recv_1, recv_2, recv_z1, recv_z2, res,
               ld_sem, g_sem, ws_sem, wr_sem, s_sem, r_sem, dw_sem, out_sem):
    z, y, f = lax.axis_index("dp"), lax.axis_index("row"), lax.axis_index("fsdp")
    x, c = f // 2, f % 2
    z0 = z % 2
    act = (z0 + c + 1) % 2
    tile = xv.shape[0] // TILES
    wide = w13.shape[2] // 2
    half_w2 = w2.shape[1] // 2
    rows = gbuf.shape[1]
    rh = rows // 2
    inner = (z + 1) // 2 % 2

    def dev(dz=None, yy=None, xx=None, cc=None):
        zz = z if dz is None else dz
        return (zz, y if yy is None else yy, (x if xx is None else xx) * 2 + (c if cc is None else cc))

    partner = dev(cc=1 - c)
    x_nbr, y_nbr = dev(xx=1 - x), dev(yy=1 - y)
    z_near = dev(dz=z + 1 - 2 * z0)
    z_mirror = dev(dz=3 - z)

    own_loads = [pltpu.make_async_copy(s, d, ld_sem.at[i]) for i, (s, d) in enumerate(((wg_hbm, w13.at[0, :, pl.ds(0, wide)]), (wu_hbm, w13.at[0, :, pl.ds(wide, wide)]), (wd_hbm, w2.at[0])))]
    act_loads = [pltpu.make_async_copy(s, d, ld_sem.at[3 + i]) for i, (s, d) in enumerate(((x_hbm, xv), (dy_hbm, dyv)))]
    for cp in own_loads + act_loads:
        cp.start()

    def g_load(k):
        return pltpu.make_async_copy(g_hbm.at[k], gbuf.at[k % 3], g_sem.at[k % 3])

    g_load(0).start()
    g_load(1).start()

    barrier = pltpu.get_barrier_semaphore()
    for d in (partner, x_nbr, y_nbr, z_near, z_mirror):
        pl.semaphore_signal(barrier, inc=1, device_id=d, device_id_type=pl.DeviceIdType.MESH)
    pl.semaphore_wait(barrier, 5)

    def part(slot, p):
        if p < 2:
            return w13.at[slot, :, pl.ds(p * wide, wide)]
        return w2.at[slot, pl.ds((p - 2) * half_w2, half_w2)]

    def wcopy(src, dst, p, sem, device):
        return pltpu.make_async_remote_copy(
            src_ref=part(src, p), dst_ref=part(dst, p), send_sem=ws_sem.at[sem, p], recv_sem=wr_sem.at[dst, p],
            device_id=device, device_id_type=pl.DeviceIdType.MESH)

    def wwait(slot, p):
        wcopy(slot, slot, p, 0, partner).wait_recv()

    def own_copies():
        return [wcopy(0, 1, p, 0, partner) for p in range(4)]

    def own_far():
        return [wcopy(0, s, p, i, d) for p in range(4) for s, i, d in ((2, 1, x_nbr), (3, 2, y_nbr))]

    def z_x(p):
        return wcopy(2, 2, p, 3, z_near)

    def z_y(p):
        return wcopy(3, 3, p, 4, z_near)

    def take_x(p):
        return [wcopy(2, 5, p, 5, partner)] + ([wcopy(2, 4, p, 7, y_nbr)] if p % 2 == 0 else [])

    def take_y(p):
        return [wcopy(3, 6, p, 6, partner)] + ([wcopy(3, 4, p, 7, x_nbr)] if p % 2 == 1 else [])

    def take_d(p):
        return [wcopy(4, 7, p, 8, partner)]

    fetch, relay = {}, {}
    for p in range(4):
        fetch.setdefault(TAKE_XY[p], []).append((2, functools.partial(take_x, p), p))
        fetch.setdefault(TAKE_XY[p], []).append((3, functools.partial(take_y, p), p))
        for units, make in ((Z_X, z_x), (Z_Y, z_y)):
            fetch.setdefault(units[p], []).append((None, lambda p=p, make=make: [make(p)], p))
        relay.setdefault(PASS_X[p], []).append((2, functools.partial(take_x, p), p))
        relay.setdefault(PASS_Y[p], []).append((3, functools.partial(take_y, p), p))
        fetch.setdefault(TAKE_D[p], []).append((4, functools.partial(take_d, p), p))
        relay.setdefault(PASS_D[p], []).append((4, functools.partial(take_d, p), p))

    for cp in own_loads:
        cp.wait()
    for cp in own_copies():
        cp.start()

    @pl.when(act == 1)
    def _():
        for cp in own_far():
            cp.start()

    for cp in act_loads:
        cp.wait()

    def neighbour(k, stage):
        typ = (k + stage) % 2
        return dev(yy=(y + typ) % 2, xx=(x + 1 - typ) % 2)

    def rcopy(stage, k, src, dst, device):
        return pltpu.make_async_remote_copy(
            src_ref=src, dst_ref=dst, send_sem=s_sem.at[stage, k % SLOTS], recv_sem=r_sem.at[stage, k],
            device_id=device, device_id_type=pl.DeviceIdType.MESH)

    def half(other=0):
        return pl.ds(pl.multiple_of((z + 1 + other) % 2 * rh, rh), rh)

    def stage_copy(stage, k):
        if stage == 0:
            return rcopy(0, k, send_c.at[k % SLOTS], recv_c.at[k], partner)
        if stage == 1:
            return rcopy(1, k, own.at[k, pl.ds(2, 2)], recv_1.at[k], neighbour(k, 0))
        if stage == 2:
            return rcopy(2, k, own.at[k, 1], recv_2.at[k], neighbour(k, 1))
        if stage == 3:
            return rcopy(3, k, own.at[k, 0], recv_z1.at[k], z_near)
        if stage == 4:
            return rcopy(4, k, own.at[k, 0, half(1)], recv_z2.at[k], z_mirror)
        if stage == 5:
            return rcopy(5, k, res.at[k, half()], res.at[k, half()], z_mirror)
        at = half(stage - 6)
        return rcopy(stage, k, res.at[k, at], res.at[k, at], z_near)

    def free_slot(stage, k):
        @pl.when(k >= SLOTS)
        def _():
            stage_copy(stage, k - SLOTS).wait_send()

    def add(p, q):
        return (p.astype(F32) + q.astype(F32)).astype(BF16)

    def start(stage, k):
        free_slot(stage, k)
        stage_copy(stage, k).start()

    def event(stage, k):
        if stage > 0:
            stage_copy(stage - 1, k).wait_recv()
        if stage == 0:
            free_slot(0, k)
            typ = k % 2
            g_load(k).wait()

            @pl.when(k + 2 < CHUNKS)
            def _():
                g_load(k + 2).start()

            for a in range(2):
                for b in range(2):
                    xx = (x + a + (b - a) * typ) % 2
                    yy = (y + b + (a - b) * typ) % 2
                    block = yy * 4 + xx * 2
                    send_c[k % SLOTS, 2 * a + b] = gbuf[k % 3, :, pl.ds(pl.multiple_of((block + 1 - c) * wide, wide), wide)].astype(BF16)
                    own[k, 2 * a + b] = gbuf[k % 3, :, pl.ds(pl.multiple_of((block + c) * wide, wide), wide)].astype(BF16)
            stage_copy(0, k).start()
        elif stage == 1:
            own[k] = add(own[k], recv_c[k])
            start(1, k)
        elif stage == 2:
            own[k, 0:2] = add(own[k, 0:2], recv_1[k])
            start(2, k)
        elif stage == 3:
            own[k, 0] = add(own[k, 0], recv_2[k])

            @pl.when(inner == 0)
            def _():
                start(3, k)
        elif stage == 4:
            own[k, 0] = add(own[k, 0], recv_z1[k])
            start(4, k)
        elif stage == 5:
            res[k, half()] = add(own[k, 0, half()], recv_z2[k])
            start(5, k)
            start(6, k)
        else:
            start(7, k)

    def reduce_events(u):
        for stage in range(6, -1, -1):
            k = u - FIRST - LAGS[stage]
            here = (k >= 0) & (k < CHUNKS)

            @pl.when(here if stage < 4 else here & (inner == 1))
            def _(stage=stage, k=k):
                event(stage, k)

    def weight_events(u):
        for mine, table in ((1, fetch), (0, relay)):
            for group in sorted({t // GROUP for t in table}):
                @pl.when((u // GROUP == group) & (act == mine))
                def _(table=table, group=group):
                    for t in sorted(t for t in table if t // GROUP == group):
                        @pl.when(u == t)
                        def _(t=t):
                            for slot, make, p in table[t]:
                                if slot is not None:
                                    wwait(slot, p)
                                for cp in make():
                                    cp.start()

    def slot_of(i):
        return jnp.where(i < 2, i, 2 + (i + 1 + 3 * (1 - act) + 3) % 6)

    def column_of(slot):
        b = jnp.where(slot < 5, slot, slot - 3)
        dc = jnp.where((slot == 1) | (slot >= 5), 1, 0)
        ddx = jnp.where((b == 2) | (b == 4), 1, 0)
        ddy = jnp.where((b == 3) | (b == 4), 1, 0)
        return ((y + ddy) % 2) * 4 + ((x + ddx) % 2) * 2 + (c + dc) % 2

    def dw_copy(i):
        at = pl.ds(pl.multiple_of(column_of(slot_of(i)) * wide, wide), wide)
        return pltpu.make_async_copy(dwacc.at[i % 2], dw_out.at[:, :, at], dw_sem.at[i % 2])

    def dx_copy(m):
        at = pl.ds(pl.multiple_of(m * tile, tile), tile)
        return pltpu.make_async_copy(xv.at[at], dx_out.at[at], out_sem.at[m])

    dot = functools.partial(lax.dot_general, preferred_element_type=F32)

    def rows_of(m):
        return pl.ds(pl.multiple_of(m * tile, tile), tile)

    def before(u):
        weight_events(u)
        reduce_events(u)
        i, m = u // TILES, u % TILES
        slot = slot_of(i)

        @pl.when((m == 0) & ((slot == 1) | (slot >= 5)))
        def _():
            for p in range(4):
                wwait(slot, p)

        @pl.when(i == 0)
        def _():
            xt[m] = xv[rows_of(m)].T
            dyt[m] = dyv[rows_of(m)].T

        @pl.when((m == 1) & (i >= 2))
        def _():
            dw_copy(i - 2).wait()

    def products(u):
        slot, at = slot_of(u // TILES), rows_of(u % TILES)
        half = tile // 2
        first = pl.multiple_of((u % TILES) * tile, tile)
        dh = [dot(dyv[pl.ds(first + n * half, half)], w2[slot], LAST) for n in range(2)]
        return dot(xv[at], w13[slot], FIRST_TO_LAST), jnp.concatenate(dh, axis=0)

    def gate(ab, dh, dab, h):
        a, b = ab[:, :wide], ab[:, wide:]
        s = jax.nn.sigmoid(a)
        silu = a * s
        h[...] = (silu * b).astype(BF16)
        dab[:, :wide] = (dh * b * s * (1.0 + a * (1.0 - s))).astype(BF16)
        dab[:, wide:] = (dh * silu).astype(BF16)

    def gradients(u, dab, h):
        i, m = u // TILES, u % TILES
        d = i % 2
        half, dim = tile // 2, xt.shape[1] // 2
        first = pl.multiple_of(m * tile, tile)
        for n in range(2):
            at = pl.ds(n * dim, dim)
            dwacc[d, 2, at] = jnp.where(m == 0, 0.0, dwacc[d, 2, at]) + dot(dyt[m, at], h[...], FIRST_TO_LAST)
        for n in range(2):
            at = pl.ds(first + n * half, half)
            dxacc[at] = jnp.where(i == 0, 0.0, dxacc[at]) + dot(dab[n * half:(n + 1) * half], w13[slot_of(i)], LAST)
        for n in range(2):
            at = pl.ds(n * dim, dim)
            left = dot(xt[m, at], dab[...], FIRST_TO_LAST)
            dwacc[d, 0, at] = jnp.where(m == 0, 0.0, dwacc[d, 0, at]) + left[:, :wide]
            dwacc[d, 1, at] = jnp.where(m == 0, 0.0, dwacc[d, 1, at]) + left[:, wide:]

    def after(u):
        i, m = u // TILES, u % TILES

        @pl.when(m == TILES - 1)
        def _():
            dw_copy(i).start()

        @pl.when(i == BLOCKS - 1)
        def _():
            at = rows_of(m)
            xv[at] = dxacc[at].astype(BF16)
            dx_copy(m).start()

    even, odd = (dab_even, h_even), (dab_odd, h_odd)

    def step(u, now, last):
        before(u)
        ab, dh = products(u)
        gradients(u - 1, *last)
        gate(ab, dh, *now)
        after(u - 1)

    def body(v, carry):
        step(2 * v + 1, odd, even)
        step(2 * v + 2, even, odd)
        return carry

    def tail(u, carry):
        reduce_events(u)
        return carry

    before(0)
    gate(*products(0), *even)
    lax.fori_loop(0, UNITS // 2 - 1, body, 0)
    step(UNITS - 1, odd, even)
    reduce_events(UNITS)
    gradients(UNITS - 1, *odd)
    after(UNITS - 1)
    lax.fori_loop(UNITS + 1, FIRST + CHUNKS + LAGS[-1], tail, 0)

    @pl.when(inner == 0)
    def _():
        for k in range(CHUNKS):
            stage_copy(6, k).wait_recv()
            stage_copy(7, k).wait_recv()

    store = pltpu.make_async_copy(res, dn_out, ld_sem.at[0])
    store.start()

    for cp in own_copies():
        cp.wait_send()

    @pl.when(act == 1)
    def _():
        for cp in own_far():
            cp.wait_send()
        for p in range(4):
            z_x(p).wait_send()
            z_y(p).wait_send()

    for p in range(4):
        for cp in take_x(p) + take_y(p) + take_d(p):
            cp.wait_send()
    def drain(*stages):
        for stage in stages:
            for k in range(CHUNKS - SLOTS, CHUNKS):
                stage_copy(stage, k).wait_send()

    drain(0, 1, 2)

    @pl.when(inner == 0)
    def _():
        drain(3)

    @pl.when(inner == 1)
    def _():
        drain(4, 5, 6, 7)

    dw_copy(BLOCKS - 2).wait()
    dw_copy(BLOCKS - 1).wait()
    for m in range(TILES):
        dx_copy(m).wait()
    store.wait()


def solution(mesh):
    def per_device(x_blk, dy_blk, gate, up, down, g_part):
        tokens, dim = x_blk.shape
        wide = gate.shape[1]
        hidden = wide * BLOCKS
        rows = 3 * dim // CHUNKS
        tile = tokens // TILES
        g = g_part.reshape(CHUNKS, rows, hidden)
        vm = pltpu.VMEM
        dma = pltpu.SemaphoreType.DMA
        dx, dn, dw = pl.pallas_call(
            whole_step,
            out_shape=[
                jax.ShapeDtypeStruct((tokens, dim), BF16),
                jax.ShapeDtypeStruct((CHUNKS, rows, wide), BF16),
                jax.ShapeDtypeStruct((3, dim, hidden), F32),
            ],
            in_specs=[pl.BlockSpec(memory_space=pl.ANY)] * 6,
            out_specs=[pl.BlockSpec(memory_space=pl.ANY)] * 3,
            scratch_shapes=[
                vm((tokens, dim), BF16), vm((tokens, dim), BF16),
                vm((TILES, dim, tile), BF16), vm((TILES, dim, tile), BF16),
                vm((BLOCKS, dim, 2 * wide), BF16), vm((BLOCKS, wide, dim), BF16),
                vm((tile, 2 * wide), BF16), vm((tile, 2 * wide), BF16), vm((tile, wide), BF16), vm((tile, wide), BF16),
                vm((tokens, dim), F32), vm((2, 3, dim, wide), F32),
                vm((3, rows, hidden), F32),
                vm((SLOTS, 4, rows, wide), BF16), vm((CHUNKS, 4, rows, wide), BF16), vm((CHUNKS, 4, rows, wide), BF16),
                vm((CHUNKS, 2, rows, wide), BF16), vm((CHUNKS, rows, wide), BF16),
                vm((CHUNKS, rows, wide), BF16), vm((CHUNKS, rows // 2, wide), BF16), vm((CHUNKS, rows, wide), BF16),
                dma((5,)), dma((3,)), dma((10, 4)), dma((BLOCKS, 4)), dma((8, SLOTS)), dma((8, CHUNKS)), dma((2,)), dma((TILES,)),
            ],
            compiler_params=pltpu.CompilerParams(collective_id=0, has_side_effects=True, vmem_limit_bytes=67043328),
            cost_estimate=pl.CostEstimate(flops=16 * tokens * dim * hidden, bytes_accessed=60 << 20, transcendentals=tokens * hidden),
        )(x_blk, dy_blk, gate, up, down, g)
        return dx, dn.reshape(3, dim, wide).astype(F32), dw[None]

    return jax.shard_map(
        per_device,
        mesh=mesh,
        in_specs=(P(ALL_AXES, None), P(ALL_AXES, None), P(None, GROUP_AXES), P(None, GROUP_AXES), P(GROUP_AXES, None), P(ALL_AXES, None, None, None)),
        out_specs=(P(ALL_AXES, None), P(None, None, GROUP_AXES), P(ALL_AXES, None, None, None)),
        check_vma=False,
    )
```

```python
import functools

import jax
import jax.numpy as jnp
from jax import lax
from jax.experimental import pallas as pl
from jax.experimental.pallas import tpu as pltpu
from jax.sharding import PartitionSpec as P

ALL_AXES = ("dp", "row", "fsdp")
GROUP_AXES = ("row", "fsdp")
LAST = (((1,), (1,)), ((), ()))
FIRST_TO_LAST = (((1,), (0,)), ((), ()))
F32, BF16 = jnp.float32, jnp.bfloat16

BLOCKS = 8
TILES = 4
UNITS = BLOCKS * TILES
KEPT = 5
LATE = BLOCKS - KEPT
CHUNKS = 18
EXPORT = 10
FIRST = 1
LAGS = (0, 1, 4, 7, 11, 13, 15)
TAKE_XY, TAKE_D = (2, 3, 4, 6), (10, 11, 14, 14)
Z_X, Z_Y = (2, 3, 4, 6), (4, 6, 10, 15)
PASS_X, PASS_Y, PASS_D = (10, 10, 13, 13), (14, 14, 16, 17), (22, 25, 27, 27)
GROUP = 4
SLOTS = 4


def slot_at(i, act):
    return jnp.where(i < 2, i, 2 + (i + 4 + 3 * (1 - act)) % 6)


def column_at(slot, x, y, c):
    b = jnp.where(slot < 5, slot, slot - 3)
    dc = jnp.where((slot == 1) | (slot >= 5), 1, 0)
    ddx = jnp.where((b == 2) | (b == 4), 1, 0)
    ddy = jnp.where((b == 3) | (b == 4), 1, 0)
    return ((y + ddy) % 2) * 4 + ((x + ddx) % 2) * 2 + (c + dc) % 2


def finish(dx_in, dn_in, dw_in, dab_in, h_in, xt_in, dyt_in, dx_out, dn_out, dw_out,
           dxv, dnb, dnf, slab, acc, dab, h, xt, dyt, in_sem, slab_sem, late_sem, out_sem):
    z, y, f = lax.axis_index("dp"), lax.axis_index("row"), lax.axis_index("fsdp")
    x, c = f // 2, f % 2
    act = (z % 2 + c + 1) % 2
    wide = slab.shape[3]

    def columns(i):
        return pl.ds(pl.multiple_of(column_at(slot_at(i, act), x, y, c) * wide, wide), wide)

    def load_late(n):
        at = pl.ds(n * TILES, TILES)
        return [pltpu.make_async_copy(dab_in.at[at], dab.at[at], late_sem.at[0, n]), pltpu.make_async_copy(h_in.at[at], h.at[at], late_sem.at[1, n])]

    def load_slab(i):
        return pltpu.make_async_copy(dw_in.at[:, :, columns(i)], slab.at[i], slab_sem.at[i])

    def store(i):
        source = slab.at[i] if i < KEPT else acc.at[i - KEPT]
        return pltpu.make_async_copy(source, dw_out.at[:, :, columns(i)], out_sem.at[i])

    left = [pltpu.make_async_copy(xt_in, xt, in_sem.at[0]), pltpu.make_async_copy(dyt_in, dyt, in_sem.at[1])]
    dx_load, dn_load = pltpu.make_async_copy(dx_in, dxv, in_sem.at[2]), pltpu.make_async_copy(dn_in, dnb, in_sem.at[3])
    dx_store, dn_store = pltpu.make_async_copy(dxv, dx_out, out_sem.at[BLOCKS]), pltpu.make_async_copy(dnf, dn_out, out_sem.at[BLOCKS + 1])
    for cp in left + load_late(0) + [load_slab(0), load_slab(1)] + load_late(1) + [load_slab(2)] + load_late(2) + [load_slab(3), load_slab(4), dx_load, dn_load]:
        cp.start()
    for cp in left:
        cp.wait()
    for n in range(LATE):
        for cp in load_late(n):
            cp.wait()

        def tile_step(m, carry, n=n):
            for a in range(2):
                at = pl.ds(a * (xt.shape[1] // 2), xt.shape[1] // 2)
                both = jnp.dot(xt[m, at], dab[n * TILES + m], preferred_element_type=F32)
                third = jnp.dot(dyt[m, at], h[n * TILES + m], preferred_element_type=F32)
                for t, part in enumerate((both[:, :wide], both[:, wide:], third)):
                    acc[n, t, at] = jnp.where(m == 0, 0.0, acc[n, t, at]) + part
            return carry

        lax.fori_loop(0, TILES, tile_step, 0)
        store(KEPT + n).start()
        for i in range(2 * n, min(2 * n + 2, KEPT)):
            load_slab(i).wait()
            store(i).start()
    dx_load.wait()
    dx_store.start()
    dn_load.wait()

    def widen(k, carry):
        dnf[k] = dnb[k].astype(F32)
        return carry

    lax.fori_loop(0, CHUNKS, widen, 0)
    dn_store.start()
    for i in range(BLOCKS):
        store(i).wait()
    dx_store.wait()
    dn_store.wait()


def whole_step(x_hbm, dy_hbm, wg_hbm, wu_hbm, wd_hbm, g_hbm, dx_out, dn_out, dw_out, dab_out, h_out, xt_out, dyt_out,
               xv, dyv, xt, dyt, w13, w2, dab_even, dab_odd, h_even, h_odd, dxacc, dwacc,
               gbuf, send_c, own, recv_c, recv_1, recv_2, recv_z1, recv_z2, res,
               ld_sem, g_sem, ws_sem, wr_sem, s_sem, r_sem, dw_sem, out_sem, keep_sem, ex_sem):
    z, y, f = lax.axis_index("dp"), lax.axis_index("row"), lax.axis_index("fsdp")
    x, c = f // 2, f % 2
    z0 = z % 2
    act = (z0 + c + 1) % 2
    tile = xv.shape[0] // TILES
    wide = w13.shape[2] // 2
    half_w2 = w2.shape[1] // 2
    rows = gbuf.shape[1]
    rh = rows // 2
    inner = (z + 1) // 2 % 2

    def dev(dz=None, yy=None, xx=None, cc=None):
        zz = z if dz is None else dz
        return (zz, y if yy is None else yy, (x if xx is None else xx) * 2 + (c if cc is None else cc))

    partner = dev(cc=1 - c)
    x_nbr, y_nbr = dev(xx=1 - x), dev(yy=1 - y)
    z_near = dev(dz=z + 1 - 2 * z0)
    z_mirror = dev(dz=3 - z)

    own_loads = [pltpu.make_async_copy(s, d, ld_sem.at[i]) for i, (s, d) in enumerate(((wg_hbm, w13.at[0, :, pl.ds(0, wide)]), (wu_hbm, w13.at[0, :, pl.ds(wide, wide)]), (wd_hbm, w2.at[0])))]
    act_loads = [pltpu.make_async_copy(s, d, ld_sem.at[3 + i]) for i, (s, d) in enumerate(((x_hbm, xv), (dy_hbm, dyv)))]
    for cp in own_loads + act_loads:
        cp.start()

    def g_load(k):
        return pltpu.make_async_copy(g_hbm.at[k], gbuf.at[k % 3], g_sem.at[k % 3])

    g_load(0).start()
    g_load(1).start()

    barrier = pltpu.get_barrier_semaphore()
    for d in (partner, x_nbr, y_nbr, z_near, z_mirror):
        pl.semaphore_signal(barrier, inc=1, device_id=d, device_id_type=pl.DeviceIdType.MESH)
    pl.semaphore_wait(barrier, 5)

    def part(slot, p):
        if p < 2:
            return w13.at[slot, :, pl.ds(p * wide, wide)]
        return w2.at[slot, pl.ds((p - 2) * half_w2, half_w2)]

    def wcopy(src, dst, p, sem, device):
        return pltpu.make_async_remote_copy(
            src_ref=part(src, p), dst_ref=part(dst, p), send_sem=ws_sem.at[sem, p], recv_sem=wr_sem.at[dst, p],
            device_id=device, device_id_type=pl.DeviceIdType.MESH)

    def wwait(slot, p):
        wcopy(slot, slot, p, 0, partner).wait_recv()

    def own_copies():
        return [wcopy(0, 1, p, 0, partner) for p in range(4)]

    def own_far():
        return [wcopy(0, s, p, i, d) for p in range(4) for s, i, d in ((2, 1, x_nbr), (3, 2, y_nbr))]

    def z_x(p):
        return wcopy(2, 2, p, 3, z_near)

    def z_y(p):
        return wcopy(3, 3, p, 4, z_near)

    def take_x(p):
        return [wcopy(2, 5, p, 5, partner)] + ([wcopy(2, 4, p, 7, y_nbr)] if p % 2 == 0 else [])

    def take_y(p):
        return [wcopy(3, 6, p, 6, partner)] + ([wcopy(3, 4, p, 7, x_nbr)] if p % 2 == 1 else [])

    def take_d(p):
        return [wcopy(4, 7, p, 8, partner)]

    fetch, relay = {}, {}
    for p in range(4):
        fetch.setdefault(TAKE_XY[p], []).append((2, functools.partial(take_x, p), p))
        fetch.setdefault(TAKE_XY[p], []).append((3, functools.partial(take_y, p), p))
        for units, make in ((Z_X, z_x), (Z_Y, z_y)):
            fetch.setdefault(units[p], []).append((None, lambda p=p, make=make: [make(p)], p))
        relay.setdefault(PASS_X[p], []).append((2, functools.partial(take_x, p), p))
        relay.setdefault(PASS_Y[p], []).append((3, functools.partial(take_y, p), p))
        fetch.setdefault(TAKE_D[p], []).append((4, functools.partial(take_d, p), p))
        relay.setdefault(PASS_D[p], []).append((4, functools.partial(take_d, p), p))

    for cp in own_loads:
        cp.wait()
    for cp in own_copies():
        cp.start()

    @pl.when(act == 1)
    def _():
        for cp in own_far():
            cp.start()

    for cp in act_loads:
        cp.wait()

    def neighbour(k, stage):
        typ = (k + stage) % 2
        return dev(yy=(y + typ) % 2, xx=(x + 1 - typ) % 2)

    def rcopy(stage, k, src, dst, device):
        return pltpu.make_async_remote_copy(
            src_ref=src, dst_ref=dst, send_sem=s_sem.at[stage, k % SLOTS], recv_sem=r_sem.at[stage, k],
            device_id=device, device_id_type=pl.DeviceIdType.MESH)

    def half(other=0):
        return pl.ds(pl.multiple_of((z + 1 + other) % 2 * rh, rh), rh)

    def stage_copy(stage, k):
        if stage == 0:
            return rcopy(0, k, send_c.at[k % SLOTS], recv_c.at[k], partner)
        if stage == 1:
            return rcopy(1, k, own.at[k, pl.ds(2, 2)], recv_1.at[k], neighbour(k, 0))
        if stage == 2:
            return rcopy(2, k, own.at[k, 1], recv_2.at[k], neighbour(k, 1))
        if stage == 3:
            return rcopy(3, k, own.at[k, 0], recv_z1.at[k], z_near)
        if stage == 4:
            return rcopy(4, k, own.at[k, 0, half(1)], recv_z2.at[k], z_mirror)
        if stage == 5:
            return rcopy(5, k, res.at[k, half()], res.at[k, half()], z_mirror)
        at = half(stage - 6)
        return rcopy(stage, k, res.at[k, at], res.at[k, at], z_near)

    def free_slot(stage, k):
        @pl.when(k >= SLOTS)
        def _():
            stage_copy(stage, k - SLOTS).wait_send()

    def add(p, q):
        return (p.astype(F32) + q.astype(F32)).astype(BF16)

    def start(stage, k):
        free_slot(stage, k)
        stage_copy(stage, k).start()

    def event(stage, k):
        if stage > 0:
            stage_copy(stage - 1, k).wait_recv()
        if stage == 0:
            free_slot(0, k)
            typ = k % 2
            g_load(k).wait()

            @pl.when(k + 2 < CHUNKS)
            def _():
                g_load(k + 2).start()

            for a in range(2):
                for b in range(2):
                    xx = (x + a + (b - a) * typ) % 2
                    yy = (y + b + (a - b) * typ) % 2
                    block = yy * 4 + xx * 2
                    send_c[k % SLOTS, 2 * a + b] = gbuf[k % 3, :, pl.ds(pl.multiple_of((block + 1 - c) * wide, wide), wide)].astype(BF16)
                    own[k, 2 * a + b] = gbuf[k % 3, :, pl.ds(pl.multiple_of((block + c) * wide, wide), wide)].astype(BF16)
            stage_copy(0, k).start()
        elif stage == 1:
            own[k] = add(own[k], recv_c[k])
            start(1, k)
        elif stage == 2:
            own[k, 0:2] = add(own[k, 0:2], recv_1[k])
            start(2, k)
        elif stage == 3:
            own[k, 0] = add(own[k, 0], recv_2[k])

            @pl.when(inner == 0)
            def _():
                start(3, k)
        elif stage == 4:
            own[k, 0] = add(own[k, 0], recv_z1[k])
            start(4, k)
        elif stage == 5:
            res[k, half()] = add(own[k, 0, half()], recv_z2[k])
            start(5, k)
            start(6, k)
        else:
            start(7, k)

    def reduce_events(u):
        for stage in range(6, -1, -1):
            k = u - FIRST - LAGS[stage]
            here = (k >= 0) & (k < CHUNKS)

            @pl.when(here if stage < 4 else here & (inner == 1))
            def _(stage=stage, k=k):
                event(stage, k)

    def weight_events(u):
        for mine, table in ((1, fetch), (0, relay)):
            for group in sorted({t // GROUP for t in table}):
                @pl.when((u // GROUP == group) & (act == mine))
                def _(table=table, group=group):
                    for t in sorted(t for t in table if t // GROUP == group):
                        @pl.when(u == t)
                        def _(t=t):
                            for slot, make, p in table[t]:
                                if slot is not None:
                                    wwait(slot, p)
                                for cp in make():
                                    cp.start()

    def slot_of(i):
        return slot_at(i, act)

    def column_of(slot):
        return column_at(slot, x, y, c)

    def dw_copy(i):
        at = pl.ds(pl.multiple_of(column_of(slot_of(i)) * wide, wide), wide)
        return pltpu.make_async_copy(dwacc.at[i % 2], dw_out.at[:, :, at], dw_sem.at[i % 2])

    def dx_copy(m):
        at = pl.ds(pl.multiple_of(m * tile, tile), tile)
        return pltpu.make_async_copy(xv.at[at], dx_out.at[at], out_sem.at[m])

    dot = functools.partial(lax.dot_general, preferred_element_type=F32)

    def rows_of(m):
        return pl.ds(pl.multiple_of(m * tile, tile), tile)

    def before(u):
        weight_events(u)
        reduce_events(u)
        i, m = u // TILES, u % TILES
        slot = slot_of(i)

        @pl.when((m == 0) & ((slot == 1) | (slot >= 5)))
        def _():
            for p in range(4):
                wwait(slot, p)

        @pl.when(i == 0)
        def _():
            xt[m] = xv[rows_of(m)].T
            dyt[m] = dyv[rows_of(m)].T

        @pl.when((m == 1) & (i >= 2) & (i < KEPT + 2))
        def _():
            dw_copy(i - 2).wait()

        @pl.when(u == EXPORT)
        def _():
            for cp in exports:
                cp.start()

    def products(u):
        slot, at = slot_of(u // TILES), rows_of(u % TILES)
        half = tile // 2
        first = pl.multiple_of((u % TILES) * tile, tile)
        dh = [dot(dyv[pl.ds(first + n * half, half)], w2[slot], LAST) for n in range(2)]
        return dot(xv[at], w13[slot], FIRST_TO_LAST), jnp.concatenate(dh, axis=0)

    def gate(ab, dh, dab, h):
        a, b = ab[:, :wide], ab[:, wide:]
        s = jax.nn.sigmoid(a)
        silu = a * s
        h[...] = (silu * b).astype(BF16)
        dab[:, :wide] = (dh * b * s * (1.0 + a * (1.0 - s))).astype(BF16)
        dab[:, wide:] = (dh * silu).astype(BF16)

    exports = [pltpu.make_async_copy(xt, xt_out, ex_sem.at[0]), pltpu.make_async_copy(dyt, dyt_out, ex_sem.at[1])]

    def keep(u, parity):
        dab, h = (even, odd)[parity]
        n = u - KEPT * TILES
        return [pltpu.make_async_copy(dab, dab_out.at[n], keep_sem.at[0, parity]), pltpu.make_async_copy(h, h_out.at[n], keep_sem.at[1, parity])]

    def gradients(u, dab, h, late=False):
        i, m = u // TILES, u % TILES
        d = i % 2
        half, dim = tile // 2, xt.shape[1] // 2
        first = pl.multiple_of(m * tile, tile)
        if not late:
            for n in range(2):
                at = pl.ds(n * dim, dim)
                dwacc[d, 2, at] = jnp.where(m == 0, 0.0, dwacc[d, 2, at]) + dot(dyt[m, at], h[...], FIRST_TO_LAST)
        for n in range(2):
            at = pl.ds(first + n * half, half)
            dxacc[at] = jnp.where(i == 0, 0.0, dxacc[at]) + dot(dab[n * half:(n + 1) * half], w13[slot_of(i)], LAST)
        if not late:
            for n in range(2):
                at = pl.ds(n * dim, dim)
                left = dot(xt[m, at], dab[...], FIRST_TO_LAST)
                dwacc[d, 0, at] = jnp.where(m == 0, 0.0, dwacc[d, 0, at]) + left[:, :wide]
                dwacc[d, 1, at] = jnp.where(m == 0, 0.0, dwacc[d, 1, at]) + left[:, wide:]

    def after(u):
        i, m = u // TILES, u % TILES

        @pl.when((m == TILES - 1) & (i < KEPT))
        def _():
            dw_copy(i).start()

        @pl.when(i == BLOCKS - 1)
        def _():
            at = rows_of(m)
            xv[at] = dxacc[at].astype(BF16)
            dx_copy(m).start()

    even, odd = (dab_even, h_even), (dab_odd, h_odd)

    def step(u, parity, late=False):
        now, last = (even, odd)[parity], (even, odd)[1 - parity]
        before(u)
        if late:
            @pl.when(u >= KEPT * TILES + 2)
            def _():
                for cp in keep(u - 2, parity):
                    cp.wait()
            for cp in keep(u - 1, 1 - parity):
                cp.start()
        ab, dh = products(u)
        gradients(u - 1, *last, late)
        gate(ab, dh, *now)
        after(u - 1)

    def body(v, carry):
        step(2 * v + 1, 1)
        step(2 * v + 2, 0)
        return carry

    def late_body(v, carry):
        step(2 * v + 1, 1, True)
        step(2 * v + 2, 0, True)
        return carry

    def tail(u, carry):
        reduce_events(u)
        return carry

    before(0)
    gate(*products(0), *even)
    lax.fori_loop(0, KEPT * TILES // 2, body, 0)
    lax.fori_loop(KEPT * TILES // 2, UNITS // 2 - 1, late_body, 0)
    step(UNITS - 1, 1, True)
    for cp in keep(UNITS - 1, 1):
        cp.start()
    reduce_events(UNITS)
    gradients(UNITS - 1, *odd, True)
    after(UNITS - 1)
    lax.fori_loop(UNITS + 1, FIRST + CHUNKS + LAGS[-1], tail, 0)

    @pl.when(inner == 0)
    def _():
        for k in range(CHUNKS):
            stage_copy(6, k).wait_recv()
            stage_copy(7, k).wait_recv()

    store = pltpu.make_async_copy(res, dn_out, ld_sem.at[0])
    store.start()

    for cp in own_copies():
        cp.wait_send()

    @pl.when(act == 1)
    def _():
        for cp in own_far():
            cp.wait_send()
        for p in range(4):
            z_x(p).wait_send()
            z_y(p).wait_send()

    for p in range(4):
        for cp in take_x(p) + take_y(p) + take_d(p):
            cp.wait_send()
    def drain(*stages):
        for stage in stages:
            for k in range(CHUNKS - SLOTS, CHUNKS):
                stage_copy(stage, k).wait_send()

    drain(0, 1, 2)

    @pl.when(inner == 0)
    def _():
        drain(3)

    @pl.when(inner == 1)
    def _():
        drain(4, 5, 6, 7)

    for cp in keep(UNITS - 2, 0) + keep(UNITS - 1, 1) + exports:
        cp.wait()
    for m in range(TILES):
        dx_copy(m).wait()
    store.wait()


def solution(mesh):
    def per_device(x_blk, dy_blk, gate, up, down, g_part):
        tokens, dim = x_blk.shape
        wide = gate.shape[1]
        hidden = wide * BLOCKS
        rows = 3 * dim // CHUNKS
        tile = tokens // TILES
        g = g_part.reshape(CHUNKS, rows, hidden)
        vm = pltpu.VMEM
        dma = pltpu.SemaphoreType.DMA
        made = pl.pallas_call(
            whole_step,
            out_shape=[
                jax.ShapeDtypeStruct((tokens, dim), BF16),
                jax.ShapeDtypeStruct((CHUNKS, rows, wide), BF16),
                jax.ShapeDtypeStruct((3, dim, hidden), F32),
                jax.ShapeDtypeStruct((LATE * TILES, tile, 2 * wide), BF16),
                jax.ShapeDtypeStruct((LATE * TILES, tile, wide), BF16),
                jax.ShapeDtypeStruct((TILES, dim, tile), BF16),
                jax.ShapeDtypeStruct((TILES, dim, tile), BF16),
            ],
            in_specs=[pl.BlockSpec(memory_space=pl.ANY)] * 6,
            out_specs=[pl.BlockSpec(memory_space=pl.ANY)] * 7,
            scratch_shapes=[
                vm((tokens, dim), BF16), vm((tokens, dim), BF16),
                vm((TILES, dim, tile), BF16), vm((TILES, dim, tile), BF16),
                vm((BLOCKS, dim, 2 * wide), BF16), vm((BLOCKS, wide, dim), BF16),
                vm((tile, 2 * wide), BF16), vm((tile, 2 * wide), BF16), vm((tile, wide), BF16), vm((tile, wide), BF16),
                vm((tokens, dim), F32), vm((2, 3, dim, wide), F32),
                vm((3, rows, hidden), F32),
                vm((SLOTS, 4, rows, wide), BF16), vm((CHUNKS, 4, rows, wide), BF16), vm((CHUNKS, 4, rows, wide), BF16),
                vm((CHUNKS, 2, rows, wide), BF16), vm((CHUNKS, rows, wide), BF16),
                vm((CHUNKS, rows, wide), BF16), vm((CHUNKS, rows // 2, wide), BF16), vm((CHUNKS, rows, wide), BF16),
                dma((5,)), dma((3,)), dma((10, 4)), dma((BLOCKS, 4)), dma((8, SLOTS)), dma((8, CHUNKS)), dma((2,)), dma((TILES,)), dma((2, 2)), dma((2,)),
            ],
            compiler_params=pltpu.CompilerParams(collective_id=0, has_side_effects=True, vmem_limit_bytes=67043328),
            cost_estimate=pl.CostEstimate(flops=16 * tokens * dim * hidden, bytes_accessed=60 << 20, transcendentals=tokens * hidden),
        )(x_blk, dy_blk, gate, up, down, g)
        dx, dn, dw = pl.pallas_call(
            finish,
            out_shape=[
                jax.ShapeDtypeStruct((tokens, dim), BF16),
                jax.ShapeDtypeStruct((CHUNKS, rows, wide), F32),
                jax.ShapeDtypeStruct((3, dim, hidden), F32),
            ],
            in_specs=[pl.BlockSpec(memory_space=pl.ANY)] * 7,
            out_specs=[pl.BlockSpec(memory_space=pl.ANY)] * 3,
            scratch_shapes=[
                vm((tokens, dim), BF16), vm((CHUNKS, rows, wide), BF16), vm((CHUNKS, rows, wide), F32),
                vm((KEPT, 3, dim, wide), F32), vm((LATE, 3, dim, wide), F32),
                vm((LATE * TILES, tile, 2 * wide), BF16), vm((LATE * TILES, tile, wide), BF16),
                vm((TILES, dim, tile), BF16), vm((TILES, dim, tile), BF16),
                dma((4,)), dma((KEPT,)), dma((2, LATE)), dma((BLOCKS + 2,)),
            ],
            compiler_params=pltpu.CompilerParams(vmem_limit_bytes=67043328),
            cost_estimate=pl.CostEstimate(flops=2 * tokens * dim * hidden, bytes_accessed=56 << 20, transcendentals=0),
        )(*made)
        return dx, dn.reshape(3, dim, wide), dw[None]

    return jax.shard_map(
        per_device,
        mesh=mesh,
        in_specs=(P(ALL_AXES, None), P(ALL_AXES, None), P(None, GROUP_AXES), P(None, GROUP_AXES), P(GROUP_AXES, None), P(ALL_AXES, None, None, None)),
        out_specs=(P(ALL_AXES, None), P(None, None, GROUP_AXES), P(ALL_AXES, None, None, None)),
        check_vma=False,
    )
```

```python
import functools

import jax
import jax.numpy as jnp
from jax import lax
from jax.experimental import pallas as pl
from jax.experimental.pallas import tpu as pltpu
from jax.sharding import PartitionSpec as P

ALL_AXES = ("dp", "row", "fsdp")
GROUP_AXES = ("row", "fsdp")
LAST = (((1,), (1,)), ((), ()))
FIRST_TO_LAST = (((1,), (0,)), ((), ()))
F32, BF16 = jnp.float32, jnp.bfloat16

BLOCKS = 8
TILES = 4
UNITS = BLOCKS * TILES
KEPT = 5
LATE = BLOCKS - KEPT
CHUNKS = 18
EXPORT = 10
FIRST = 1
LAGS = (0, 1, 5, 9, 12, 14, 16)
TAKE_XY, TAKE_D = (2, 3, 5, 7), (9, 12, 12, 13)
Z_X, Z_Y = (2, 3, 5, 9), (3, 3, 7, 12)
PASS_X, PASS_Y, PASS_D = (8, 8, 12, 12), (13, 13, 15, 16), (20, 23, 26, 26)
GROUP = 4
SLOTS = 4


def slot_at(i, act):
    return jnp.where(i < 2, i, 2 + (i + 4 + 3 * (1 - act)) % 6)


def column_at(slot, x, y, c):
    b = jnp.where(slot < 5, slot, slot - 3)
    dc = jnp.where((slot == 1) | (slot >= 5), 1, 0)
    ddx = jnp.where((b == 2) | (b == 4), 1, 0)
    ddy = jnp.where((b == 3) | (b == 4), 1, 0)
    return ((y + ddy) % 2) * 4 + ((x + ddx) % 2) * 2 + (c + dc) % 2


def finish(dx_in, dn_in, dw_in, dab_in, h_in, xt_in, dyt_in, dx_out, dn_out, dw_out,
           dxv, dnb, dnf, slab, acc, dab, h, xt, dyt, in_sem, slab_sem, late_sem, out_sem):
    z, y, f = lax.axis_index("dp"), lax.axis_index("row"), lax.axis_index("fsdp")
    x, c = f // 2, f % 2
    act = (z % 2 + c + 1) % 2
    wide = slab.shape[3]

    def columns(i):
        return pl.ds(pl.multiple_of(column_at(slot_at(i, act), x, y, c) * wide, wide), wide)

    def load_late(n):
        at = pl.ds(n * TILES, TILES)
        return [pltpu.make_async_copy(dab_in.at[at], dab.at[at], late_sem.at[0, n]), pltpu.make_async_copy(h_in.at[at], h.at[at], late_sem.at[1, n])]

    def load_slab(i):
        return pltpu.make_async_copy(dw_in.at[:, :, columns(i)], slab.at[i], slab_sem.at[i])

    def store(i):
        source = slab.at[i] if i < KEPT else acc.at[i - KEPT]
        return pltpu.make_async_copy(source, dw_out.at[:, :, columns(i)], out_sem.at[i])

    left = [pltpu.make_async_copy(xt_in, xt, in_sem.at[0]), pltpu.make_async_copy(dyt_in, dyt, in_sem.at[1])]
    dx_load, dn_load = pltpu.make_async_copy(dx_in, dxv, in_sem.at[2]), pltpu.make_async_copy(dn_in, dnb, in_sem.at[3])
    dx_store, dn_store = pltpu.make_async_copy(dxv, dx_out, out_sem.at[BLOCKS]), pltpu.make_async_copy(dnf, dn_out, out_sem.at[BLOCKS + 1])
    for cp in left + load_late(0) + [load_slab(0), load_slab(1)] + load_late(1) + [load_slab(2)] + load_late(2) + [load_slab(3), load_slab(4), dx_load, dn_load]:
        cp.start()
    for cp in left:
        cp.wait()
    for n in range(LATE):
        for cp in load_late(n):
            cp.wait()

        def tile_step(m, carry, n=n):
            for a in range(2):
                at = pl.ds(a * (xt.shape[1] // 2), xt.shape[1] // 2)
                both = jnp.dot(xt[m, at], dab[n * TILES + m], preferred_element_type=F32)
                third = jnp.dot(dyt[m, at], h[n * TILES + m], preferred_element_type=F32)
                for t, part in enumerate((both[:, :wide], both[:, wide:], third)):
                    acc[n, t, at] = jnp.where(m == 0, 0.0, acc[n, t, at]) + part
            return carry

        lax.fori_loop(0, TILES, tile_step, 0)
        store(KEPT + n).start()
        for i in range(2 * n, min(2 * n + 2, KEPT)):
            load_slab(i).wait()
            store(i).start()
    dx_load.wait()
    dx_store.start()
    dn_load.wait()

    def widen(k, carry):
        dnf[k] = dnb[k].astype(F32)
        return carry

    lax.fori_loop(0, CHUNKS, widen, 0)
    dn_store.start()
    for i in range(BLOCKS):
        store(i).wait()
    dx_store.wait()
    dn_store.wait()


def whole_step(x_hbm, dy_hbm, wg_hbm, wu_hbm, wd_hbm, g_hbm, dx_out, dn_out, dw_out, dab_out, h_out, xt_out, dyt_out,
               xv, dyv, xt, dyt, w13, w2, dab_even, dab_odd, h_even, h_odd, dxacc, dwacc,
               gbuf, send_c, own, recv_c, recv_1, recv_2, recv_z1, recv_z2, res,
               ld_sem, g_sem, ws_sem, wr_sem, s_sem, r_sem, dw_sem, out_sem, keep_sem, ex_sem):
    z, y, f = lax.axis_index("dp"), lax.axis_index("row"), lax.axis_index("fsdp")
    x, c = f // 2, f % 2
    z0 = z % 2
    act = (z0 + c + 1) % 2
    tile = xv.shape[0] // TILES
    wide = w13.shape[2] // 2
    half_w2 = w2.shape[1] // 2
    rows = gbuf.shape[1]
    rh = rows // 2
    inner = (z + 1) // 2 % 2

    def dev(dz=None, yy=None, xx=None, cc=None):
        zz = z if dz is None else dz
        return (zz, y if yy is None else yy, (x if xx is None else xx) * 2 + (c if cc is None else cc))

    partner = dev(cc=1 - c)
    x_nbr, y_nbr = dev(xx=1 - x), dev(yy=1 - y)
    z_near = dev(dz=z + 1 - 2 * z0)
    z_mirror = dev(dz=3 - z)

    own_loads = [pltpu.make_async_copy(s, d, ld_sem.at[i]) for i, (s, d) in enumerate(((wg_hbm, w13.at[0, :, pl.ds(0, wide)]), (wu_hbm, w13.at[0, :, pl.ds(wide, wide)]), (wd_hbm, w2.at[0])))]
    act_loads = [pltpu.make_async_copy(s, d, ld_sem.at[3 + i]) for i, (s, d) in enumerate(((x_hbm, xv), (dy_hbm, dyv)))]
    for cp in own_loads + act_loads:
        cp.start()

    def g_load(k):
        return pltpu.make_async_copy(g_hbm.at[k], gbuf.at[k % 3], g_sem.at[k % 3])

    g_load(0).start()
    g_load(1).start()

    barrier = pltpu.get_barrier_semaphore()
    for d in (partner, x_nbr, y_nbr, z_near, z_mirror):
        pl.semaphore_signal(barrier, inc=1, device_id=d, device_id_type=pl.DeviceIdType.MESH)
    pl.semaphore_wait(barrier, 5)

    def part(slot, p):
        if p < 2:
            return w13.at[slot, :, pl.ds(p * wide, wide)]
        return w2.at[slot, pl.ds((p - 2) * half_w2, half_w2)]

    def wcopy(src, dst, p, sem, device):
        return pltpu.make_async_remote_copy(
            src_ref=part(src, p), dst_ref=part(dst, p), send_sem=ws_sem.at[sem, p], recv_sem=wr_sem.at[dst, p],
            device_id=device, device_id_type=pl.DeviceIdType.MESH)

    def wwait(slot, p):
        wcopy(slot, slot, p, 0, partner).wait_recv()

    def own_copies():
        return [wcopy(0, 1, p, 0, partner) for p in range(4)]

    def own_far():
        return [wcopy(0, s, p, i, d) for p in range(4) for s, i, d in ((2, 1, x_nbr), (3, 2, y_nbr))]

    def z_x(p):
        return wcopy(2, 2, p, 3, z_near)

    def z_y(p):
        return wcopy(3, 3, p, 4, z_near)

    def take_x(p):
        return [wcopy(2, 5, p, 5, partner)] + ([wcopy(2, 4, p, 7, y_nbr)] if p % 2 == 0 else [])

    def take_y(p):
        return [wcopy(3, 6, p, 6, partner)] + ([wcopy(3, 4, p, 7, x_nbr)] if p % 2 == 1 else [])

    def take_d(p):
        return [wcopy(4, 7, p, 8, partner)]

    fetch, relay = {}, {}
    for p in range(4):
        fetch.setdefault(TAKE_XY[p], []).append((2, functools.partial(take_x, p), p))
        fetch.setdefault(TAKE_XY[p], []).append((3, functools.partial(take_y, p), p))
        for units, make in ((Z_X, z_x), (Z_Y, z_y)):
            fetch.setdefault(units[p], []).append((None, lambda p=p, make=make: [make(p)], p))
        relay.setdefault(PASS_X[p], []).append((2, functools.partial(take_x, p), p))
        relay.setdefault(PASS_Y[p], []).append((3, functools.partial(take_y, p), p))
        fetch.setdefault(TAKE_D[p], []).append((4, functools.partial(take_d, p), p))
        relay.setdefault(PASS_D[p], []).append((4, functools.partial(take_d, p), p))

    for cp in own_loads:
        cp.wait()
    for cp in own_copies():
        cp.start()

    @pl.when(act == 1)
    def _():
        for cp in own_far():
            cp.start()

    for cp in act_loads:
        cp.wait()

    def neighbour(k, stage):
        typ = (k + stage) % 2
        return dev(yy=(y + typ) % 2, xx=(x + 1 - typ) % 2)

    def rcopy(stage, k, src, dst, device):
        return pltpu.make_async_remote_copy(
            src_ref=src, dst_ref=dst, send_sem=s_sem.at[stage, k % SLOTS], recv_sem=r_sem.at[stage, k],
            device_id=device, device_id_type=pl.DeviceIdType.MESH)

    def half(other=0):
        return pl.ds(pl.multiple_of((z + 1 + other) % 2 * rh, rh), rh)

    def stage_copy(stage, k):
        if stage == 0:
            return rcopy(0, k, send_c.at[k % SLOTS], recv_c.at[k], partner)
        if stage == 1:
            return rcopy(1, k, own.at[k, pl.ds(2, 2)], recv_1.at[k], neighbour(k, 0))
        if stage == 2:
            return rcopy(2, k, own.at[k, 1], recv_2.at[k], neighbour(k, 1))
        if stage == 3:
            return rcopy(3, k, own.at[k, 0], recv_z1.at[k], z_near)
        if stage == 4:
            return rcopy(4, k, own.at[k, 0, half(1)], recv_z2.at[k], z_mirror)
        if stage == 5:
            return rcopy(5, k, res.at[k, half()], res.at[k, half()], z_mirror)
        at = half(stage - 6)
        return rcopy(stage, k, res.at[k, at], res.at[k, at], z_near)

    def free_slot(stage, k):
        @pl.when(k >= SLOTS)
        def _():
            stage_copy(stage, k - SLOTS).wait_send()

    def add(p, q):
        return (p.astype(F32) + q.astype(F32)).astype(BF16)

    def start(stage, k):
        free_slot(stage, k)
        stage_copy(stage, k).start()

    def event(stage, k):
        if stage > 0:
            stage_copy(stage - 1, k).wait_recv()
        if stage == 0:
            free_slot(0, k)
            typ = k % 2
            g_load(k).wait()

            @pl.when(k + 2 < CHUNKS)
            def _():
                g_load(k + 2).start()

            for a in range(2):
                for b in range(2):
                    xx = (x + a + (b - a) * typ) % 2
                    yy = (y + b + (a - b) * typ) % 2
                    block = yy * 4 + xx * 2
                    send_c[k % SLOTS, 2 * a + b] = gbuf[k % 3, :, pl.ds(pl.multiple_of((block + 1 - c) * wide, wide), wide)].astype(BF16)
                    own[k, 2 * a + b] = gbuf[k % 3, :, pl.ds(pl.multiple_of((block + c) * wide, wide), wide)].astype(BF16)
            stage_copy(0, k).start()
        elif stage == 1:
            own[k] = add(own[k], recv_c[k])
            start(1, k)
        elif stage == 2:
            own[k, 0:2] = add(own[k, 0:2], recv_1[k])
            start(2, k)
        elif stage == 3:
            own[k, 0] = add(own[k, 0], recv_2[k])

            @pl.when(inner == 0)
            def _():
                start(3, k)
        elif stage == 4:
            own[k, 0] = add(own[k, 0], recv_z1[k])
            start(4, k)
        elif stage == 5:
            res[k, half()] = add(own[k, 0, half()], recv_z2[k])
            start(5, k)
            start(6, k)
        else:
            start(7, k)

    def reduce_events(u):
        for stage in range(6, -1, -1):
            k = u - FIRST - LAGS[stage]
            here = (k >= 0) & (k < CHUNKS)

            @pl.when(here if stage < 4 else here & (inner == 1))
            def _(stage=stage, k=k):
                event(stage, k)

    def weight_events(u):
        for mine, table in ((1, fetch), (0, relay)):
            for group in sorted({t // GROUP for t in table}):
                @pl.when((u // GROUP == group) & (act == mine))
                def _(table=table, group=group):
                    for t in sorted(t for t in table if t // GROUP == group):
                        @pl.when(u == t)
                        def _(t=t):
                            for slot, make, p in table[t]:
                                if slot is not None:
                                    wwait(slot, p)
                                for cp in make():
                                    cp.start()

    def slot_of(i):
        return slot_at(i, act)

    def column_of(slot):
        return column_at(slot, x, y, c)

    def dw_copy(i):
        at = pl.ds(pl.multiple_of(column_of(slot_of(i)) * wide, wide), wide)
        return pltpu.make_async_copy(dwacc.at[i % 2], dw_out.at[:, :, at], dw_sem.at[i % 2])

    def dx_copy(m):
        at = pl.ds(pl.multiple_of(m * tile, tile), tile)
        return pltpu.make_async_copy(xv.at[at], dx_out.at[at], out_sem.at[m])

    dot = functools.partial(lax.dot_general, preferred_element_type=F32)

    def rows_of(m):
        return pl.ds(pl.multiple_of(m * tile, tile), tile)

    def before(u):
        weight_events(u)
        reduce_events(u)
        i, m = u // TILES, u % TILES
        slot = slot_of(i)

        @pl.when((m == 0) & ((slot == 1) | (slot >= 5)))
        def _():
            for p in range(4):
                wwait(slot, p)

        @pl.when(i == 0)
        def _():
            xt[m] = xv[rows_of(m)].T
            dyt[m] = dyv[rows_of(m)].T

        @pl.when((m == 1) & (i >= 2) & (i < KEPT + 2))
        def _():
            dw_copy(i - 2).wait()

        @pl.when(u == EXPORT)
        def _():
            for cp in exports:
                cp.start()

    def products(u):
        slot, at = slot_of(u // TILES), rows_of(u % TILES)
        half = tile // 2
        first = pl.multiple_of((u % TILES) * tile, tile)
        dh = [dot(dyv[pl.ds(first + n * half, half)], w2[slot], LAST) for n in range(2)]
        return dot(xv[at], w13[slot], FIRST_TO_LAST), jnp.concatenate(dh, axis=0)

    def gate(ab, dh, dab, h):
        a, b = ab[:, :wide], ab[:, wide:]
        s = jax.nn.sigmoid(a)
        silu = a * s
        h[...] = (silu * b).astype(BF16)
        dab[:, :wide] = (dh * b * s * (1.0 + a * (1.0 - s))).astype(BF16)
        dab[:, wide:] = (dh * silu).astype(BF16)

    exports = [pltpu.make_async_copy(xt, xt_out, ex_sem.at[0]), pltpu.make_async_copy(dyt, dyt_out, ex_sem.at[1])]

    def keep(u, parity):
        dab, h = (even, odd)[parity]
        n = u - KEPT * TILES
        return [pltpu.make_async_copy(dab, dab_out.at[n], keep_sem.at[0, parity]), pltpu.make_async_copy(h, h_out.at[n], keep_sem.at[1, parity])]

    def gradients(u, dab, h, late=False):
        i, m = u // TILES, u % TILES
        d = i % 2
        half, dim = tile // 2, xt.shape[1] // 2
        first = pl.multiple_of(m * tile, tile)
        if not late:
            for n in range(2):
                at = pl.ds(n * dim, dim)
                dwacc[d, 2, at] = jnp.where(m == 0, 0.0, dwacc[d, 2, at]) + dot(dyt[m, at], h[...], FIRST_TO_LAST)
        for n in range(2):
            at = pl.ds(first + n * half, half)
            dxacc[at] = jnp.where(i == 0, 0.0, dxacc[at]) + dot(dab[n * half:(n + 1) * half], w13[slot_of(i)], LAST)
        if not late:
            for n in range(2):
                at = pl.ds(n * dim, dim)
                left = dot(xt[m, at], dab[...], FIRST_TO_LAST)
                dwacc[d, 0, at] = jnp.where(m == 0, 0.0, dwacc[d, 0, at]) + left[:, :wide]
                dwacc[d, 1, at] = jnp.where(m == 0, 0.0, dwacc[d, 1, at]) + left[:, wide:]

    def after(u):
        i, m = u // TILES, u % TILES

        @pl.when((m == TILES - 1) & (i < KEPT))
        def _():
            dw_copy(i).start()

        @pl.when(i == BLOCKS - 1)
        def _():
            at = rows_of(m)
            xv[at] = dxacc[at].astype(BF16)
            dx_copy(m).start()

    even, odd = (dab_even, h_even), (dab_odd, h_odd)

    def step(u, parity, late=False):
        now, last = (even, odd)[parity], (even, odd)[1 - parity]
        before(u)
        if late:
            @pl.when(u >= KEPT * TILES + 2)
            def _():
                for cp in keep(u - 2, parity):
                    cp.wait()
            for cp in keep(u - 1, 1 - parity):
                cp.start()
        ab, dh = products(u)
        gradients(u - 1, *last, late)
        gate(ab, dh, *now)
        after(u - 1)

    def body(v, carry):
        step(2 * v + 1, 1)
        step(2 * v + 2, 0)
        return carry

    def late_body(v, carry):
        step(2 * v + 1, 1, True)
        step(2 * v + 2, 0, True)
        return carry

    def tail(u, carry):
        reduce_events(u)
        return carry

    before(0)
    gate(*products(0), *even)
    lax.fori_loop(0, KEPT * TILES // 2, body, 0)
    lax.fori_loop(KEPT * TILES // 2, UNITS // 2 - 1, late_body, 0)
    step(UNITS - 1, 1, True)
    for cp in keep(UNITS - 1, 1):
        cp.start()
    reduce_events(UNITS)
    gradients(UNITS - 1, *odd, True)
    after(UNITS - 1)
    lax.fori_loop(UNITS + 1, FIRST + CHUNKS + LAGS[-1], tail, 0)

    @pl.when(inner == 0)
    def _():
        for k in range(CHUNKS):
            stage_copy(6, k).wait_recv()
            stage_copy(7, k).wait_recv()

    store = pltpu.make_async_copy(res, dn_out, ld_sem.at[0])
    store.start()

    for cp in own_copies():
        cp.wait_send()

    @pl.when(act == 1)
    def _():
        for cp in own_far():
            cp.wait_send()
        for p in range(4):
            z_x(p).wait_send()
            z_y(p).wait_send()

    for p in range(4):
        for cp in take_x(p) + take_y(p) + take_d(p):
            cp.wait_send()
    def drain(*stages):
        for stage in stages:
            for k in range(CHUNKS - SLOTS, CHUNKS):
                stage_copy(stage, k).wait_send()

    drain(0, 1, 2)

    @pl.when(inner == 0)
    def _():
        drain(3)

    @pl.when(inner == 1)
    def _():
        drain(4, 5, 6, 7)

    for cp in keep(UNITS - 2, 0) + keep(UNITS - 1, 1) + exports:
        cp.wait()
    for m in range(TILES):
        dx_copy(m).wait()
    store.wait()


def solution(mesh):
    def per_device(x_blk, dy_blk, gate, up, down, g_part):
        tokens, dim = x_blk.shape
        wide = gate.shape[1]
        hidden = wide * BLOCKS
        rows = 3 * dim // CHUNKS
        tile = tokens // TILES
        g = g_part.reshape(CHUNKS, rows, hidden)
        vm = pltpu.VMEM
        dma = pltpu.SemaphoreType.DMA
        made = pl.pallas_call(
            whole_step,
            out_shape=[
                jax.ShapeDtypeStruct((tokens, dim), BF16),
                jax.ShapeDtypeStruct((CHUNKS, rows, wide), BF16),
                jax.ShapeDtypeStruct((3, dim, hidden), F32),
                jax.ShapeDtypeStruct((LATE * TILES, tile, 2 * wide), BF16),
                jax.ShapeDtypeStruct((LATE * TILES, tile, wide), BF16),
                jax.ShapeDtypeStruct((TILES, dim, tile), BF16),
                jax.ShapeDtypeStruct((TILES, dim, tile), BF16),
            ],
            in_specs=[pl.BlockSpec(memory_space=pl.ANY)] * 6,
            out_specs=[pl.BlockSpec(memory_space=pl.ANY)] * 7,
            scratch_shapes=[
                vm((tokens, dim), BF16), vm((tokens, dim), BF16),
                vm((TILES, dim, tile), BF16), vm((TILES, dim, tile), BF16),
                vm((BLOCKS, dim, 2 * wide), BF16), vm((BLOCKS, wide, dim), BF16),
                vm((tile, 2 * wide), BF16), vm((tile, 2 * wide), BF16), vm((tile, wide), BF16), vm((tile, wide), BF16),
                vm((tokens, dim), F32), vm((2, 3, dim, wide), F32),
                vm((3, rows, hidden), F32),
                vm((SLOTS, 4, rows, wide), BF16), vm((CHUNKS, 4, rows, wide), BF16), vm((CHUNKS, 4, rows, wide), BF16),
                vm((CHUNKS, 2, rows, wide), BF16), vm((CHUNKS, rows, wide), BF16),
                vm((CHUNKS, rows, wide), BF16), vm((CHUNKS, rows // 2, wide), BF16), vm((CHUNKS, rows, wide), BF16),
                dma((5,)), dma((3,)), dma((10, 4)), dma((BLOCKS, 4)), dma((8, SLOTS)), dma((8, CHUNKS)), dma((2,)), dma((TILES,)), dma((2, 2)), dma((2,)),
            ],
            compiler_params=pltpu.CompilerParams(collective_id=0, has_side_effects=True, vmem_limit_bytes=67043328),
            cost_estimate=pl.CostEstimate(flops=16 * tokens * dim * hidden, bytes_accessed=60 << 20, transcendentals=tokens * hidden),
        )(x_blk, dy_blk, gate, up, down, g)
        dx, dn, dw = pl.pallas_call(
            finish,
            out_shape=[
                jax.ShapeDtypeStruct((tokens, dim), BF16),
                jax.ShapeDtypeStruct((CHUNKS, rows, wide), F32),
                jax.ShapeDtypeStruct((3, dim, hidden), F32),
            ],
            in_specs=[pl.BlockSpec(memory_space=pl.ANY)] * 7,
            out_specs=[pl.BlockSpec(memory_space=pl.ANY)] * 3,
            scratch_shapes=[
                vm((tokens, dim), BF16), vm((CHUNKS, rows, wide), BF16), vm((CHUNKS, rows, wide), F32),
                vm((KEPT, 3, dim, wide), F32), vm((LATE, 3, dim, wide), F32),
                vm((LATE * TILES, tile, 2 * wide), BF16), vm((LATE * TILES, tile, wide), BF16),
                vm((TILES, dim, tile), BF16), vm((TILES, dim, tile), BF16),
                dma((4,)), dma((KEPT,)), dma((2, LATE)), dma((BLOCKS + 2,)),
            ],
            compiler_params=pltpu.CompilerParams(vmem_limit_bytes=67043328),
            cost_estimate=pl.CostEstimate(flops=2 * tokens * dim * hidden, bytes_accessed=56 << 20, transcendentals=0),
        )(*made)
        return dx, dn.reshape(3, dim, wide), dw[None]

    return jax.shard_map(
        per_device,
        mesh=mesh,
        in_specs=(P(ALL_AXES, None), P(ALL_AXES, None), P(None, GROUP_AXES), P(None, GROUP_AXES), P(GROUP_AXES, None), P(ALL_AXES, None, None, None)),
        out_specs=(P(ALL_AXES, None), P(None, None, GROUP_AXES), P(ALL_AXES, None, None, None)),
        check_vma=False,
    )
```
